32 devices in a mesh: ka: 16 (over z, x, core), sp: 2 (over y).
Axes of the slice: x: 2, y: 2, z: 4, core: 2. Of those that a mesh axis runs over, the one named last changes fastest.
Arguments:
- bloch_index: int32 [16, 2], P('ka'), may hold values from 0 to 63
- material: int32 [32, 64, 128], P('sp'), may hold values from 0 to 2
- permittivity: float32 [3], replicated, may hold values from 1 to 12
- absorption_peak: float32 [1], replicated, may hold values from 0.25 to 2
- source_sheet: float32 [16, 2, 32, 64], P('ka', None, 'sp'), may hold values from -6 to 6
- waveform: float32 [10], replicated, may hold values from -6 to 6
- electric_in: bfloat16 [16, 6, 32, 64, 128], P('ka', None, 'sp'), may hold values from -12 to 12
- magnetic_in: bfloat16 [16, 6, 32, 64, 128], P('ka', None, 'sp'), may hold values from -12 to 12
Outputs:
- electric_out: float32 [16, 6, 32, 64, 128], P('ka', None, 'sp')
- magnetic_out: float32 [16, 6, 32, 64, 128], P('ka', None, 'sp')
- reflected: float32 [16, 2], P('ka')
- reflected_mean: float32 [2], replicated
The draws below stay inside these ranges and needn't reach their ends.
All inputs are finite; a program needn't handle non-finite values.
Results may differ from the reference program's by a relative error of at most 0.0003.
Values sent between devices are 32-bit elements; how exact they have to be, the bound alone decides.
No kernel may reach another device: no remote copies, remote signals or barrier semaphores. Data moves between devices by JAX's collectives and lax.ppermute only.
A program may use at most 64 MiB of HBM per device.

```python
import math
import jax
import jax.numpy as jnp
from jax import lax

NY = 64
NZ = 128
PML = 16
STEPS = 10
INTERVAL = 5
NSNAP = 2
MPHASE = 64
NMAT = 3
K = 16
NX = 32


def start_field(key, salt):
    key = jax.random.fold_in(key, salt)
    level_key, phase_key, noise_key, common_key = jax.random.split(key, 4)
    level = jax.random.uniform(level_key, (K, 1, 1, 1, 1), jnp.float32, -1.0, 1.0)
    amplitude = jnp.exp(0.6931472 * level)
    phase = jax.random.uniform(phase_key, (K, 1, 1, 1, 1), jnp.float32, 0.0, 6.2831853)
    across = jnp.arange(NX, dtype=jnp.float32).reshape(1, 1, NX, 1, 1)
    profile = 1.0 + 0.6 * jnp.sin(6.2831853 * across / NX + phase)
    full_shape = (K, 6, NX, NY, NZ)
    rough = jnp.clip(jax.random.normal(noise_key, full_shape, jnp.float32), -3.5, 3.5)
    return (amplitude * profile * rough).astype(jnp.bfloat16)


def draw_electric_in(key, part):
    return start_field(key, 11)


def draw_magnetic_in(key, part):
    return start_field(key, 23)


def set_ends(values, rng, low, top_value):
    longest = values.shape.index(max(values.shape))
    spots = []
    for shift in (0, 1):
        where = [jax.random.randint(jax.random.fold_in(rng, axis), (), 0, length) for axis, length in enumerate(values.shape)]
        where[longest] = (where[longest] + shift) % values.shape[longest]
        spots.append(tuple(where))
    return values.at[spots[0]].set(low).at[spots[1]].set(top_value)


def block_scale(rng, dims, cuts, low, largest):
    gain = 1.0
    for position, blocks in cuts:
        heights = jax.random.uniform(jax.random.fold_in(jax.random.fold_in(rng, 6), position), (blocks,), jnp.float32, low / len(cuts), largest / len(cuts))
        gain = gain * jnp.repeat(jnp.exp(heights), dims[position] // blocks).reshape((-1,) + (1,) * (len(dims) - 1 - position))
    return gain


def normal_values(stream_key, extent, deviation, reach, shards=(), kind=jnp.bfloat16):
    values = deviation * jax.random.normal(stream_key, extent, jnp.float32)
    if shards:
        values = values * block_scale(stream_key, extent, shards, -0.22, 0.18)
    return jnp.clip(values, -reach, reach).astype(kind)


def setup_inputs(seed: int = 0) -> dict:
    keys = jax.random.split(jax.random.key(seed), 9)
    bloch_index = set_ends(jax.random.randint(keys[0], (K, 2), 0, MPHASE), jax.random.fold_in(keys[0], 1), 0, MPHASE - 1).astype(jnp.int32)
    material = set_ends(jax.random.randint(keys[1], (NX, NY, NZ), 0, NMAT), jax.random.fold_in(keys[1], 1), 0, NMAT - 1).astype(jnp.int32)
    permittivity = jnp.clip(jnp.exp(jax.random.uniform(keys[2], (NMAT,), jnp.float32, math.log(1.0), math.log(12.0))), 1.0, 12.0)
    absorption_peak = jnp.clip(jnp.exp(jax.random.uniform(keys[3], (1,), jnp.float32, math.log(0.25), math.log(2.0))), 0.25, 2.0)
    source_sheet = normal_values(keys[4], (K, 2, NX, NY), 1.0, 6.0, ((0, 16), (2, 2)), jnp.float32)
    waveform = normal_values(keys[5], (STEPS,), 1.0, 6.0, (), jnp.float32)
    electric_in = draw_electric_in(jax.random.fold_in(keys[8], 71), 0)
    magnetic_in = draw_magnetic_in(jax.random.fold_in(keys[8], 71), 0)
    return dict(bloch_index=bloch_index, material=material, permittivity=permittivity, absorption_peak=absorption_peak, source_sheet=source_sheet, waveform=waveform, electric_in=electric_in, magnetic_in=magnetic_in)


TIME_STEP = 0.5


def rotate(couple, cosine, sine):
    return (couple[0] * cosine - couple[1] * sine, couple[0] * sine + couple[1] * cosine)


def subtract(left, right):
    return (left[0] - right[0], left[1] - right[1])


def slice_along(couple, begin_at, end_at, along):
    return tuple(lax.slice_in_dim(values, begin_at, end_at, axis=along) for values in couple)


def attach(front, back, along):
    return tuple(jnp.concatenate([first_part, second_part], axis=along) for first_part, second_part in zip(front, back))


def above_cell(couple, beyond, along):
    length = couple[0].shape[along]
    return attach(slice_along(couple, 1, length, along), beyond, along)


def below_cell(couple, beyond, along):
    length = couple[0].shape[along]
    return attach(beyond, slice_along(couple, 0, length - 1, along), along)


def forward_wrap(couple, along, cosine, sine):
    beyond = rotate(slice_along(couple, 0, 1, along), cosine, sine)
    return subtract(above_cell(couple, beyond, along), couple)


def backward_wrap(couple, along, cosine, sine):
    length = couple[0].shape[along]
    beyond = rotate(slice_along(couple, length - 1, length, along), cosine, -sine)
    return subtract(couple, below_cell(couple, beyond, along))


def forward_open(couple):
    along = couple[0].ndim - 1
    beyond = tuple(jnp.zeros_like(values) for values in slice_along(couple, 0, 1, along))
    return subtract(above_cell(couple, beyond, along), couple)


def backward_open(couple):
    along = couple[0].ndim - 1
    beyond = tuple(jnp.zeros_like(values) for values in slice_along(couple, 0, 1, along))
    return subtract(couple, below_cell(couple, beyond, along))


def electric_curl(electric, beyond_y, beyond_z, cosine, sine):
    ex_part, ey_part, ez_part = electric
    across = ex_part[0].ndim - 3
    sideways = across + 1
    dx_ey = subtract(above_cell(ey_part, beyond_y, across), ey_part)
    dx_ez = subtract(above_cell(ez_part, beyond_z, across), ez_part)
    return (subtract(forward_wrap(ez_part, sideways, cosine, sine), forward_open(ey_part)),
            subtract(forward_open(ex_part), dx_ez),
            subtract(dx_ey, forward_wrap(ex_part, sideways, cosine, sine)))


def magnetic_curl(magnetic, behind_y, behind_z, cosine, sine):
    hx_part, hy_part, hz_part = magnetic
    across = hx_part[0].ndim - 3
    sideways = across + 1
    bx_hy = subtract(hy_part, below_cell(hy_part, behind_y, across))
    bx_hz = subtract(hz_part, below_cell(hz_part, behind_z, across))
    return (subtract(backward_wrap(hz_part, sideways, cosine, sine), backward_open(hy_part)),
            subtract(backward_open(hx_part), bx_hz),
            subtract(bx_hy, backward_wrap(hx_part, sideways, cosine, sine)))


def relax(couple, change, retain, factor):
    return (retain * couple[0] + factor * change[0], retain * couple[1] + factor * change[1])


def coefficients(material, permittivity, absorption_peak, depth):
    height = jnp.arange(depth, dtype=jnp.float32)
    low_depth = jnp.maximum(PML - height, 0.0) / PML
    high_depth = jnp.maximum(height - (depth - 1 - PML), 0.0) / PML
    conduct = absorption_peak[0] * (low_depth ** 3 + high_depth ** 3)
    half_mag = conduct * (0.5 * TIME_STEP)
    h_retain = (1.0 - half_mag) / (1.0 + half_mag)
    h_factor = -TIME_STEP / (1.0 + half_mag)
    relative = jnp.zeros(material.shape, jnp.float32)
    for level in range(NMAT):
        relative = relative + jnp.where(material == level, permittivity[level], 0.0)
    half_ele = conduct * (0.5 * TIME_STEP) / relative
    e_retain = (1.0 - half_ele) / (1.0 + half_ele)
    e_factor = TIME_STEP / relative / (1.0 + half_ele)
    return e_retain, e_factor, h_retain, h_factor


def reference(bloch_index, material, permittivity, absorption_peak, source_sheet, waveform, electric_in, magnetic_in):
    depth = material.shape[2]
    rows = material.shape[0]
    e_retain, e_factor, h_retain, h_factor = coefficients(material, permittivity, absorption_peak, depth)
    plane = (jnp.arange(depth) == PML + 2).astype(jnp.float32)
    monitor = PML + 6
    angles = 2.0 * jnp.pi * bloch_index.astype(jnp.float32) / MPHASE

    def one_point(inputs):
        angle_pair, sheet_pair, electric_begin, magnetic_begin = inputs
        cos_x = jnp.cos(angle_pair[0])
        sin_x = jnp.sin(angle_pair[0])
        cos_y = jnp.cos(angle_pair[1])
        sin_y = jnp.sin(angle_pair[1])
        sheet = (sheet_pair[0][:, :, None] * plane, sheet_pair[1][:, :, None] * plane)

        def advance(fields, drive):
            electric, magnetic = fields
            beyond_y = rotate(slice_along(electric[1], 0, 1, 0), cos_x, sin_x)
            beyond_z = rotate(slice_along(electric[2], 0, 1, 0), cos_x, sin_x)
            change = electric_curl(electric, beyond_y, beyond_z, cos_y, sin_y)
            magnetic = tuple(relax(couple, change_part, h_retain, h_factor) for couple, change_part in zip(magnetic, change))
            behind_y = rotate(slice_along(magnetic[1], rows - 1, rows, 0), cos_x, -sin_x)
            behind_z = rotate(slice_along(magnetic[2], rows - 1, rows, 0), cos_x, -sin_x)
            change = magnetic_curl(magnetic, behind_y, behind_z, cos_y, sin_y)
            first_change = (change[0][0] - drive * sheet[0], change[0][1] - drive * sheet[1])
            change = (first_change, change[1], change[2])
            electric = tuple(relax(couple, change_part, e_retain, e_factor) for couple, change_part in zip(electric, change))
            return (electric, magnetic)

        def snapshot(fields, index):
            fields = lax.fori_loop(0, INTERVAL, lambda inner, held: advance(held, waveform[index * INTERVAL + inner]), fields)
            electric = fields[0]
            power = (electric[0][0][:, :, monitor] ** 2 + electric[0][1][:, :, monitor] ** 2
                     + electric[1][0][:, :, monitor] ** 2 + electric[1][1][:, :, monitor] ** 2)
            return fields, jnp.sum(power) / power.size

        electric_wide = electric_begin.astype(jnp.float32)
        magnetic_wide = magnetic_begin.astype(jnp.float32)
        start_e = tuple((electric_wide[2 * member], electric_wide[2 * member + 1]) for member in range(3))
        start_h = tuple((magnetic_wide[2 * member], magnetic_wide[2 * member + 1]) for member in range(3))
        final, powers = lax.scan(snapshot, (start_e, start_h), jnp.arange(NSNAP))
        electric, magnetic = final
        electric_stack = jnp.stack([values for couple in electric for values in couple], 0)
        magnetic_stack = jnp.stack([values for couple in magnetic for values in couple], 0)
        return electric_stack, magnetic_stack, powers

    electric_out, magnetic_out, reflected = lax.map(one_point, (angles, source_sheet, electric_in, magnetic_in))
    reflected_mean = jnp.sum(reflected, 0) / reflected.shape[0]
    return electric_out, magnetic_out, reflected, reflected_mean
```

```python
import functools

import jax
import jax.numpy as jnp
from jax import lax
from jax.experimental import pallas as pl
from jax.experimental.pallas import tpu as pltpu
from jax.sharding import PartitionSpec as P

PML = 16
INTERVAL = 5
NSNAP = 2
MPHASE = 64
NMAT = 3
TIME_STEP = 0.5
SUB = 8

VMEM = pl.BlockSpec(memory_space=pltpu.VMEM)
SMEM = pl.BlockSpec(memory_space=pltpu.SMEM)
HBM = pl.BlockSpec(memory_space=pl.ANY)
F32 = jnp.float32


def load(ref, *where):
    tiles = ref.shape[-2] // SUB
    return [ref[(*where, pl.ds(SUB * j, SUB))].astype(F32) for j in range(tiles)]


def load_couple(ref, member, *where):
    return (load(ref, 2 * member, *where), load(ref, 2 * member + 1, *where))


def store(ref, values, *where):
    for j, tile in enumerate(values):
        ref[(*where, pl.ds(SUB * j, SUB))] = tile


def store_couple(ref, couple, member, *where):
    store(ref, couple[0], 2 * member, *where)
    store(ref, couple[1], 2 * member + 1, *where)


def both(fn, *couples):
    return tuple(
        [fn(*tiles) for tiles in zip(*parts)] for parts in zip(*couples)
    )


def scaled(planes, fn, couple, *others):
    out = []
    for part in range(2):
        parts = [couple[part], *(other[part] for other in others)]
        out.append([fn(*tiles) for tiles in zip(*planes, *parts)])
    return tuple(out)


def turn(couple, cosine, sine):
    return (
        [re * cosine - im * sine for re, im in zip(*couple)],
        [re * sine + im * cosine for re, im in zip(*couple)],
    )


def next_y(couple, cosine, sine):
    rows = lax.broadcasted_iota(jnp.int32, couple[0][0].shape, 0)
    wrapped = turn((couple[0][:1], couple[1][:1]), cosine, sine)
    out = []
    for part, edge in zip(couple, wrapped):
        after = part[1:] + edge
        out.append(
            [
                pltpu.roll(jnp.where(rows == 0, there, here), SUB - 1, 0)
                for here, there in zip(part, after)
            ]
        )
    return tuple(out)


def prior_y(couple, cosine, sine):
    rows = lax.broadcasted_iota(jnp.int32, couple[0][0].shape, 0)
    wrapped = turn((couple[0][-1:], couple[1][-1:]), cosine, -sine)
    out = []
    for part, edge in zip(couple, wrapped):
        before = edge + part[:-1]
        out.append(
            [
                pltpu.roll(jnp.where(rows == SUB - 1, there, here), 1, 0)
                for here, there in zip(part, before)
            ]
        )
    return tuple(out)


def next_z(couple):
    depth = couple[0][0].shape[1]
    lanes = lax.broadcasted_iota(jnp.int32, couple[0][0].shape, 1)
    return both(
        lambda tile: jnp.where(lanes == depth - 1, 0.0, pltpu.roll(tile, depth - 1, 1)),
        couple,
    )


def prior_z(couple):
    lanes = lax.broadcasted_iota(jnp.int32, couple[0][0].shape, 1)
    return both(lambda tile: jnp.where(lanes == 0, 0.0, pltpu.roll(tile, 1, 1)), couple)


def h_coefs(ref):
    return ref[0], ref[1]


def new_hx(ey, ez, hx, keep, gain, cosine, sine):
    return both(
        lambda h, z_up, z, y_up, y: keep * h + gain * ((z_up - z) - (y_up - y)),
        hx,
        next_y(ez, cosine, sine),
        ez,
        next_z(ey),
        ey,
    )


def partial_h(ex, ey, ez, hy, hz, keep, gain, cosine, sine):
    part_y = both(
        lambda h, x_up, x, z: keep * h + gain * ((x_up - x) + z), hy, next_z(ex), ex, ez
    )
    part_z = both(
        lambda h, x_up, x, y: keep * h - gain * ((x_up - x) + y),
        hz,
        next_y(ex, cosine, sine),
        ex,
        ey,
    )
    return part_y, part_z


def close_h(part_y, part_z, ey_above, ez_above, gain):
    return (
        both(lambda h, z: h - gain * z, part_y, ez_above),
        both(lambda h, y: h + gain * y, part_z, ey_above),
    )


def h_row(e_ref, h_ref, x, keep, gain, cosine, sine, with_x=True):
    ex, ey, ez = (load_couple(e_ref, m, x) for m in range(3))
    ey_above, ez_above = (load_couple(e_ref, m, x + 1) for m in (1, 2))
    hx, hy, hz = (load_couple(h_ref, m, x) for m in range(3))
    new_x = new_hx(ey, ez, hx, keep, gain, cosine, sine)
    new_y = both(
        lambda h, x_up, x_, z_up, z: keep * h + gain * ((x_up - x_) - (z_up - z)),
        hy,
        next_z(ex),
        ex,
        ez_above,
        ez,
    )
    new_z = both(
        lambda h, y_up, y, x_up, x_: keep * h + gain * ((y_up - y) - (x_up - x_)),
        hz,
        ey_above,
        ey,
        next_y(ex, cosine, sine),
        ex,
    )
    store_couple(h_ref, new_x, 0, x)
    store_couple(h_ref, new_y, 1, x)
    store_couple(h_ref, new_z, 2, x)


def new_e(e, h, hy_below, hz_below, retain, factor, sheet, drive, cosine, sine):
    ex, ey, ez = e
    hx, hy, hz = h
    drive_x = both(lambda s: drive * s, sheet)
    new_x = scaled(
        (retain, factor),
        lambda r, f, e_, z, z_dn, y, y_dn, s: r * e_ + f * ((z - z_dn) - (y - y_dn) - s),
        ex,
        hz,
        prior_y(hz, cosine, sine),
        hy,
        prior_z(hy),
        drive_x,
    )
    new_y = scaled(
        (retain, factor),
        lambda r, f, e_, x, x_dn, z, z_dn: r * e_ + f * ((x - x_dn) - (z - z_dn)),
        ey,
        hx,
        prior_z(hx),
        hz,
        hz_below,
    )
    new_z = scaled(
        (retain, factor),
        lambda r, f, e_, y, y_dn, x, x_dn: r * e_ + f * ((y - y_dn) - (x - x_dn)),
        ez,
        hy,
        hy_below,
        hx,
        prior_y(hx, cosine, sine),
    )
    return new_x, new_y, new_z


def e_row(e_ref, h_ref, c_ref, sheet_ref, x, drive, cosine, sine, below=None):
    e = [load_couple(e_ref, m, x) for m in range(3)]
    h = [load_couple(h_ref, m, x) for m in range(3)]
    if below is None:
        below = [load_couple(h_ref, m, x - 1) for m in (1, 2)]
    retain, factor = load(c_ref, 0, x), load(c_ref, 1, x)
    sheet = (load(sheet_ref, 0, x), load(sheet_ref, 1, x))
    new = new_e(e, h, *below, retain, factor, sheet, drive, cosine, sine)
    for m in range(3):
        store_couple(e_ref, new[m], m, x)
    return new


def first_kernel(bloch_ref, hc_ref, e_hbm, h_hbm, d_ref, s_ref, low, high, mag, sems):
    rows = e_hbm.shape[1]
    copies = [
        pltpu.make_async_copy(e_hbm.at[pl.ds(2, 4), 0], low, sems.at[0]),
        pltpu.make_async_copy(e_hbm.at[:, rows - 1], high, sems.at[1]),
        pltpu.make_async_copy(h_hbm.at[pl.ds(2, 4), rows - 1], mag, sems.at[2]),
    ]
    for copy in copies:
        copy.start()
    cosine, sine = bloch_ref[0], bloch_ref[1]
    keep, gain = h_coefs(hc_ref)
    copies[0].wait()
    d_ref[...] = low[...].astype(F32)
    copies[1].wait()
    copies[2].wait()
    ex, ey, ez = (load_couple(high, m) for m in range(3))
    hy, hz = (load_couple(mag, m) for m in range(2))
    part_y, part_z = partial_h(ex, ey, ez, hy, hz, keep, gain, cosine, sine)
    store_couple(s_ref, part_y, 0)
    store_couple(s_ref, part_z, 1)


def widen_kernel(peak_ref, perm_ref, mat_ref, ein_ref, hin_ref, e_ref, h_ref, c_ref):
    rows, width, depth = mat_ref.shape
    conduct = conductivity(peak_ref[0], (width, depth))

    def one_row(x, carry):
        for m in range(6):
            e_ref[m, x] = ein_ref[m, x].astype(F32)
            h_ref[m, x] = hin_ref[m, x].astype(F32)
        level = mat_ref[x]
        relative = jnp.zeros((width, depth), F32)
        for index in range(NMAT):
            relative = jnp.where(level == index, perm_ref[index], relative)
        half = conduct * (0.5 * TIME_STEP) / relative
        c_ref[0, x] = (1.0 - half) / (1.0 + half)
        c_ref[1, x] = TIME_STEP / relative / (1.0 + half)
        return carry

    lax.fori_loop(0, rows, one_row, 0)


def conductivity(peak, shape):
    depth = shape[-1]
    height = lax.broadcasted_iota(jnp.int32, shape, len(shape) - 1).astype(F32)
    low = jnp.maximum(PML - height, 0.0) / PML
    high = jnp.maximum(height - (depth - 1 - PML), 0.0) / PML
    return peak * (low * low * low + high * high * high)


def inner_kernel(
    lo, hi, step, bloch_ref, wave_ref, hc_ref, c_ref, sheet_ref, e_in, h_in, e_ref, h_ref
):
    rows = e_ref.shape[1]
    cosine, sine, drive = bloch_ref[0], bloch_ref[1], wave_ref[step]
    keep, gain = h_coefs(hc_ref)
    top = hi == rows - 1

    h_row(e_ref, h_ref, lo, keep, gain, cosine, sine)
    h_row(e_ref, h_ref, lo + 1, keep, gain, cosine, sine)

    def one_row(x, carry):
        h_row(e_ref, h_ref, x + 1, keep, gain, cosine, sine)
        e_row(e_ref, h_ref, c_ref, sheet_ref, x, drive, cosine, sine)
        return carry

    lax.fori_loop(lo + 1, hi - 1, one_row, 0)
    e_row(e_ref, h_ref, c_ref, sheet_ref, hi - 1, drive, cosine, sine)
    if top:
        ey, ez = (load_couple(e_ref, m, rows - 1) for m in (1, 2))
        hx = load_couple(h_ref, 0, rows - 1)
        store_couple(h_ref, new_hx(ey, ez, hx, keep, gain, cosine, sine), 0, rows - 1)
    else:
        e_row(e_ref, h_ref, c_ref, sheet_ref, hi, drive, cosine, sine)


def upper_kernel(
    step, bloch_ref, wave_ref, hc_ref, c_ref, sheet_ref, s_ref, d_ref, e_in, h_in,
    e_ref, h_ref, out_ref,
):
    x = e_ref.shape[1] - 1
    cosine, sine, drive = bloch_ref[0], bloch_ref[1], wave_ref[step]
    keep, gain = h_coefs(hc_ref)
    part_y, part_z = (load_couple(s_ref, m) for m in range(2))
    ey_above, ez_above = (
        turn(load_couple(d_ref, m), bloch_ref[2], bloch_ref[3]) for m in range(2)
    )
    hy, hz = close_h(part_y, part_z, ey_above, ez_above, gain)
    store_couple(h_ref, hy, 1, x)
    store_couple(h_ref, hz, 2, x)
    ex, ey, ez = e_row(e_ref, h_ref, c_ref, sheet_ref, x, drive, cosine, sine)
    part_y, part_z = partial_h(ex, ey, ez, hy, hz, keep, gain, cosine, sine)
    store_couple(out_ref, part_y, 0)
    store_couple(out_ref, part_z, 1)


def lower_kernel(
    step, bloch_ref, wave_ref, hc_ref, c_ref, sheet_ref, s_ref, e_in, h_in,
    e_ref, out_ref,
):
    cosine, sine, drive = bloch_ref[0], bloch_ref[1], wave_ref[step]
    _, gain = h_coefs(hc_ref)
    part_y, part_z = (
        turn(load_couple(s_ref, m), bloch_ref[4], bloch_ref[5]) for m in range(2)
    )
    ey, ez = (load_couple(e_ref, m, 0) for m in (1, 2))
    below = close_h(part_y, part_z, ey, ez, gain)
    _, ey, ez = e_row(e_ref, h_in, c_ref, sheet_ref, 0, drive, cosine, sine, below)
    store_couple(out_ref, ey, 0)
    store_couple(out_ref, ez, 1)


def power_kernel(slot, scale, lo, hi, e_ref, old_ref, out_ref):
    depth = e_ref.shape[-1]

    def one_row(x, total):
        for m in range(4):
            for tile in load(e_ref, m, x):
                total = total + tile * tile
        return total

    total = lax.fori_loop(lo, hi, one_row, jnp.zeros((SUB, depth), F32))
    lanes = lax.broadcasted_iota(jnp.int32, (SUB, depth), 1)
    total = jnp.where(lanes == PML + 6, total, 0.0)
    total = jnp.sum(jnp.sum(total, 0, keepdims=True), 1, keepdims=True) * scale
    out_ref[...] = old_ref[...] + jnp.where(lanes == slot, total, 0.0)


def finish_kernel(e_ref, h_ref, e_out, h_out, sems):
    copies = [
        pltpu.make_async_copy(e_ref, e_out, sems.at[0]),
        pltpu.make_async_copy(h_ref, h_out, sems.at[1]),
    ]
    for copy in copies:
        copy.start()
    for copy in copies:
        copy.wait()


def add_kernel(scale, *refs):
    total = refs[0][...]
    for ref in refs[1:-1]:
        total = total + ref[...]
    refs[-1][...] = total * scale if scale != 1.0 else total


def nbytes(shape):
    size = 4
    for extent in shape:
        size *= extent
    return size


def call(kernel, outs, ins, specs, aliases=None, scratch=(), flops=0, vmem=16):
    return pl.pallas_call(
        kernel,
        out_shape=tuple(pltpu.VMEM(shape, F32) for shape in outs),
        in_specs=specs,
        out_specs=tuple(VMEM for _ in outs),
        input_output_aliases=aliases or {},
        scratch_shapes=scratch,
        cost_estimate=pl.CostEstimate(flops=flops, bytes_accessed=0, transcendentals=0),
        compiler_params=pltpu.CompilerParams(vmem_limit_bytes=vmem * 2**20),
    )(*ins)


def shift(value, axis, steps):
    count = lax.axis_size(axis)
    return lax.ppermute(value, axis, [(i, (i + steps) % count) for i in range(count)])


def total_over(value, axis, scale=1.0):
    count = lax.axis_size(axis)
    shape = value.shape
    if count & (count - 1):
        parts = [value] + [shift(value, axis, step) for step in range(1, count)]
        return call(functools.partial(add_kernel, scale), [shape], parts, [VMEM] * count)[0]
    step = 1
    while step < count:
        other = lax.ppermute(value, axis, [(i, i ^ step) for i in range(count)])
        step *= 2
        last = scale if step >= count else 1.0
        value = call(
            functools.partial(add_kernel, last), [shape], [value, other], [VMEM] * 2
        )[0]
    return value


def on_device(
    bloch_index,
    material,
    permittivity,
    absorption_peak,
    source_sheet,
    waveform,
    electric_in,
    magnetic_in,
):
    points = bloch_index.shape[0]
    rows, width, depth = material.shape
    steps = waveform.shape[0]
    slab = lax.axis_index("sp")
    slabs = lax.axis_size("sp")
    total_points = points * lax.axis_size("ka")
    cells_plane = rows * slabs * width

    angles = 2.0 * jnp.pi * bloch_index.astype(F32) / MPHASE
    at_end = slab == slabs - 1
    at_start = slab == 0
    cosines, sines = jnp.cos(angles), jnp.sin(angles)
    half_mag = conductivity(absorption_peak[0], (SUB, depth)) * (0.5 * TIME_STEP)
    hc = jnp.stack([(1.0 - half_mag) / (1.0 + half_mag), -TIME_STEP / (1.0 + half_mag)])
    plane = (jnp.arange(depth) == PML + 2).astype(F32)
    sheets = source_sheet[..., None] * plane

    results = []
    for point in range(points):
        cos_x, cos_y = cosines[point, 0], cosines[point, 1]
        sin_x, sin_y = sines[point, 0], sines[point, 1]
        bloch = jnp.stack(
            [
                cos_y,
                sin_y,
                jnp.where(at_end, cos_x, 1.0),
                jnp.where(at_end, sin_x, 0.0),
                jnp.where(at_start, cos_x, 1.0),
                jnp.where(at_start, -sin_x, 0.0),
            ]
        )
        results.append(
            one_point(
                bloch, hc, sheets[point], waveform, material, permittivity,
                absorption_peak, electric_in[point], magnetic_in[point],
                steps, 1.0 / cells_plane,
            )
        )
    electric, magnetic, powers = zip(*results)
    sums = [total_over(power, "sp") for power in powers]
    local = sums[0]
    for other in sums[1:]:
        local = local + other
    mean = total_over(local, "ka", 1.0 / total_points)
    return (
        jnp.stack(electric),
        jnp.stack(magnetic),
        jnp.stack([total[0, :NSNAP] for total in sums]),
        mean[0, :NSNAP],
    )


def one_point(
    bloch, hc, sheet, waveform, material, permittivity, peak, electric_in, magnetic_in,
    steps, scale,
):
    rows, width, depth = material.shape
    edge = (4, width, depth)
    full = (6, rows, width, depth)
    middle = rows // 2
    mine_d, mine_s = call(
        first_kernel,
        [edge, edge],
        [bloch, hc, electric_in, magnetic_in],
        [SMEM, VMEM, HBM, HBM],
        scratch=[
            pltpu.VMEM((4, width, depth), electric_in.dtype),
            pltpu.VMEM((6, width, depth), electric_in.dtype),
            pltpu.VMEM((4, width, depth), electric_in.dtype),
            pltpu.SemaphoreType.DMA((3,)),
        ],
    )
    their_d = shift(mine_d, "sp", -1)
    their_s = shift(mine_s, "sp", 1)
    e, h, c = call(
        widen_kernel,
        [full, full, (2, rows, width, depth)],
        [peak, permittivity, material, electric_in, magnetic_in],
        [SMEM, SMEM, VMEM, VMEM, VMEM],
    )
    power = jnp.zeros((SUB, depth), F32)

    def inner(lo, hi, step, e, h):
        return call(
            functools.partial(inner_kernel, lo, hi, step),
            [full, full],
            [bloch, waveform, hc, c, sheet, e, h],
            [SMEM, SMEM] + [VMEM] * 5,
            {5: 0, 6: 1},
        )

    def measured(lo, hi, step, power, e):
        if (step + 1) % INTERVAL:
            return power
        return call(
            functools.partial(power_kernel, step // INTERVAL, scale, lo, hi),
            [(SUB, depth)],
            [e, power],
            [VMEM, VMEM],
        )[0]

    e, h = inner(middle, rows - 1, 0, e, h)
    e, h = inner(0, middle, 0, e, h)
    for step in range(steps):
        e, h, next_s = call(
            functools.partial(upper_kernel, step),
            [full, full, edge],
            [bloch, waveform, hc, c, sheet, mine_s, their_d, e, h],
            [SMEM, SMEM] + [VMEM] * 7,
            {7: 0, 8: 1},
        )
        last = step == steps - 1
        power = measured(middle + 1, rows, step, power, e)
        if not last:
            next_their_s = shift(next_s, "sp", 1)
            e, h = inner(middle, rows - 1, step + 1, e, h)
        e, mine_d = call(
            functools.partial(lower_kernel, step),
            [full, edge],
            [bloch, waveform, hc, c, sheet, their_s, e, h],
            [SMEM, SMEM] + [VMEM] * 6,
            {6: 0},
        )
        if not last:
            their_d = shift(mine_d, "sp", -1)
            mine_s, their_s = next_s, next_their_s
        power = measured(0, middle + 1, step, power, e)
        if not last:
            e, h = inner(0, middle, step + 1, e, h)
    whole = jax.ShapeDtypeStruct(full, F32)
    e, h = pl.pallas_call(
        finish_kernel,
        out_shape=(whole, whole),
        in_specs=[VMEM, VMEM],
        out_specs=(HBM, HBM),
        scratch_shapes=[pltpu.SemaphoreType.DMA((2,))],
        compiler_params=pltpu.CompilerParams(vmem_limit_bytes=2**20),
    )(e, h)
    return e, h, power


def solution(mesh):
    in_specs = (
        P("ka", None),
        P("sp", None, None),
        P(),
        P(),
        P("ka", None, "sp", None),
        P(),
        P("ka", None, "sp", None, None),
        P("ka", None, "sp", None, None),
    )
    out_specs = (
        P("ka", None, "sp", None, None),
        P("ka", None, "sp", None, None),
        P("ka", None),
        P(),
    )
    return jax.shard_map(
        on_device, mesh=mesh, in_specs=in_specs, out_specs=out_specs, check_vma=False
    )
```

```python
import functools

import jax
import jax.numpy as jnp
from jax import lax
from jax.experimental import pallas as pl
from jax.experimental.pallas import tpu as pltpu
from jax.sharding import PartitionSpec as P


PML = 16
INTERVAL = 5
NSNAP = 2
MPHASE = 64
NMAT = 3
TIME_STEP = 0.5
SUB = 8

VMEM = pl.BlockSpec(memory_space=pltpu.VMEM)
SMEM = pl.BlockSpec(memory_space=pltpu.SMEM)
HBM = pl.BlockSpec(memory_space=pltpu.HBM)
ANY = pl.BlockSpec(memory_space=pl.ANY)
F32 = jnp.float32

COS, SIN, END, START, KEEP, GAIN, DRIVE = 0, 1, 2, 4, 6, 7, 8


def load(ref, *where):
    tiles = ref.shape[-2] // SUB
    return [ref[(*where, pl.ds(SUB * j, SUB))].astype(F32) for j in range(tiles)]


def load_couple(ref, member, *where):
    return (load(ref, 2 * member, *where), load(ref, 2 * member + 1, *where))


def store(ref, values, *where):
    for j, tile in enumerate(values):
        ref[(*where, pl.ds(SUB * j, SUB))] = tile


def store_couple(ref, couple, member, *where):
    store(ref, couple[0], 2 * member, *where)
    store(ref, couple[1], 2 * member + 1, *where)


def both(fn, *couples):
    return tuple(
        [fn(*tiles) for tiles in zip(*parts)] for parts in zip(*couples)
    )


def scaled(planes, fn, couple, *others):
    out = []
    for part in range(2):
        parts = [couple[part], *(other[part] for other in others)]
        out.append([fn(*tiles) for tiles in zip(*planes, *parts)])
    return tuple(out)


def turn(couple, cosine, sine):
    return (
        [re * cosine - im * sine for re, im in zip(*couple)],
        [re * sine + im * cosine for re, im in zip(*couple)],
    )


def next_y(couple, cosine, sine):
    rows = lax.broadcasted_iota(jnp.int32, couple[0][0].shape, 0)
    wrapped = turn((couple[0][:1], couple[1][:1]), cosine, sine)
    out = []
    for part, edge in zip(couple, wrapped):
        after = part[1:] + edge
        out.append(
            [
                pltpu.roll(jnp.where(rows == 0, there, here), SUB - 1, 0)
                for here, there in zip(part, after)
            ]
        )
    return tuple(out)


def prior_y(couple, cosine, sine):
    rows = lax.broadcasted_iota(jnp.int32, couple[0][0].shape, 0)
    wrapped = turn((couple[0][-1:], couple[1][-1:]), cosine, -sine)
    out = []
    for part, edge in zip(couple, wrapped):
        before = edge + part[:-1]
        out.append(
            [
                pltpu.roll(jnp.where(rows == SUB - 1, there, here), 1, 0)
                for here, there in zip(part, before)
            ]
        )
    return tuple(out)


def next_z(couple):
    depth = couple[0][0].shape[1]
    lanes = lax.broadcasted_iota(jnp.int32, couple[0][0].shape, 1)
    return both(
        lambda tile: jnp.where(lanes == depth - 1, 0.0, pltpu.roll(tile, depth - 1, 1)),
        couple,
    )


def prior_z(couple):
    lanes = lax.broadcasted_iota(jnp.int32, couple[0][0].shape, 1)
    return both(lambda tile: jnp.where(lanes == 0, 0.0, pltpu.roll(tile, 1, 1)), couple)


def new_hx(ey, ez, hx, keep, gain, cosine, sine):
    return both(
        lambda h, z_up, z, y_up, y: keep * h + gain * ((z_up - z) - (y_up - y)),
        hx,
        next_y(ez, cosine, sine),
        ez,
        next_z(ey),
        ey,
    )


def partial_h(ex, ey, ez, hy, hz, keep, gain, cosine, sine):
    part_y = both(
        lambda h, x_up, x, z: keep * h + gain * ((x_up - x) + z), hy, next_z(ex), ex, ez
    )
    part_z = both(
        lambda h, x_up, x, y: keep * h - gain * ((x_up - x) + y),
        hz,
        next_y(ex, cosine, sine),
        ex,
        ey,
    )
    return part_y, part_z


def close_h(part_y, part_z, ey_above, ez_above, gain):
    return (
        both(lambda h, z: h - gain * z, part_y, ez_above),
        both(lambda h, y: h + gain * y, part_z, ey_above),
    )


def h_row(e_ref, h_ref, x, keep, gain, cosine, sine):
    ex, ey, ez = (load_couple(e_ref, m, x) for m in range(3))
    ey_above, ez_above = (load_couple(e_ref, m, x + 1) for m in (1, 2))
    hx, hy, hz = (load_couple(h_ref, m, x) for m in range(3))
    new_x = new_hx(ey, ez, hx, keep, gain, cosine, sine)
    new_y = both(
        lambda h, x_up, x_, z_up, z: keep * h + gain * ((x_up - x_) - (z_up - z)),
        hy,
        next_z(ex),
        ex,
        ez_above,
        ez,
    )
    new_z = both(
        lambda h, y_up, y, x_up, x_: keep * h + gain * ((y_up - y) - (x_up - x_)),
        hz,
        ey_above,
        ey,
        next_y(ex, cosine, sine),
        ex,
    )
    store_couple(h_ref, new_x, 0, x)
    store_couple(h_ref, new_y, 1, x)
    store_couple(h_ref, new_z, 2, x)


def new_e(e, h, hy_below, hz_below, retain, factor, sheet, drive, cosine, sine):
    ex, ey, ez = e
    hx, hy, hz = h
    drive_x = both(lambda s: drive * s, sheet)
    new_x = scaled(
        (retain, factor),
        lambda r, f, e_, z, z_dn, y, y_dn, s: r * e_ + f * ((z - z_dn) - (y - y_dn) - s),
        ex,
        hz,
        prior_y(hz, cosine, sine),
        hy,
        prior_z(hy),
        drive_x,
    )
    new_y = scaled(
        (retain, factor),
        lambda r, f, e_, x, x_dn, z, z_dn: r * e_ + f * ((x - x_dn) - (z - z_dn)),
        ey,
        hx,
        prior_z(hx),
        hz,
        hz_below,
    )
    new_z = scaled(
        (retain, factor),
        lambda r, f, e_, y, y_dn, x, x_dn: r * e_ + f * ((y - y_dn) - (x - x_dn)),
        ez,
        hy,
        hy_below,
        hx,
        prior_y(hx, cosine, sine),
    )
    return new_x, new_y, new_z


def e_row(e_ref, h_ref, c_ref, sheet_ref, x, drive, cosine, sine, below=None):
    e = [load_couple(e_ref, m, x) for m in range(3)]
    h = [load_couple(h_ref, m, x) for m in range(3)]
    if below is None:
        below = [load_couple(h_ref, m, x - 1) for m in (1, 2)]
    retain, factor = load(c_ref, 0, x), load(c_ref, 1, x)
    sheet = (load(sheet_ref, 0, x), load(sheet_ref, 1, x))
    new = new_e(e, h, *below, retain, factor, sheet, drive, cosine, sine)
    for m in range(3):
        store_couple(e_ref, new[m], m, x)
    return new


def is_upper(phase):
    return lax.axis_index("sp") % 2 == phase


def fetch(pairs, sems):
    copies = [
        pltpu.make_async_copy(source, target, sems.at[i])
        for i, (source, target) in enumerate(pairs)
    ]
    for copy in copies:
        copy.start()
    return copies


def first_kernel(
    bloch_hbm, peak_hbm, wave_hbm, e_hbm, h_hbm, p_ref, one_ref, two_ref,
    bloch, peak, wave, low, high, mag, sems,
):
    rows = e_hbm.shape[1]
    copies = fetch(
        [
            (bloch_hbm, bloch),
            (peak_hbm, peak),
            (wave_hbm, wave),
            (e_hbm.at[pl.ds(2, 4), 0], low),
            (e_hbm.at[:, rows - 1], high),
            (h_hbm.at[pl.ds(2, 4), rows - 1], mag),
        ],
        sems,
    )
    for copy in copies[:3]:
        copy.wait()
    shape = p_ref.shape[1:]
    angle_x, angle_y = (
        2.0 * jnp.pi * jnp.full(shape, bloch[0, axis].astype(F32)) / MPHASE
        for axis in range(2)
    )
    cos_x, sin_x = jnp.cos(angle_x), jnp.sin(angle_x)
    slab, slabs = lax.axis_index("sp"), lax.axis_size("sp")
    at_end, at_start = slab == slabs - 1, slab == 0
    half = conductivity(peak[0], shape) * (0.5 * TIME_STEP)
    p_ref[COS] = cosine = jnp.cos(angle_y)
    p_ref[SIN] = sine = jnp.sin(angle_y)
    p_ref[END] = jnp.where(at_end, cos_x, 1.0)
    p_ref[END + 1] = jnp.where(at_end, sin_x, 0.0)
    p_ref[START] = jnp.where(at_start, cos_x, 1.0)
    p_ref[START + 1] = jnp.where(at_start, -sin_x, 0.0)
    p_ref[KEEP] = keep = (1.0 - half) / (1.0 + half)
    p_ref[GAIN] = gain = -TIME_STEP / (1.0 + half)
    for step in range(wave.shape[0]):
        p_ref[DRIVE + step] = jnp.full(shape, wave[step])
    for copy in copies[3:]:
        copy.wait()

    def write(d_ref, s_ref):
        d_ref[...] = low[...].astype(F32)
        ex, ey, ez = (load_couple(high, m) for m in range(3))
        hy, hz = (load_couple(mag, m) for m in range(2))
        part_y, part_z = partial_h(ex, ey, ez, hy, hz, keep, gain, cosine, sine)
        store_couple(s_ref, part_y, 0)
        store_couple(s_ref, part_z, 1)

    @pl.when(is_upper(0))
    def _():
        write(two_ref, one_ref)

    @pl.when(jnp.logical_not(is_upper(0)))
    def _():
        write(one_ref, two_ref)


def widen_kernel(
    peak_hbm, perm_hbm, mat_hbm, e_hbm, h_hbm, e_ref, h_ref, c_ref,
    peak, perm, mat, e_in, h_in, small, sems,
):
    rows, width, depth = mat.shape
    parts = sems.shape[0]
    size = rows // parts
    scalars = fetch([(peak_hbm, peak), (perm_hbm, perm)], small)
    copies = []
    for part in range(parts):
        some = pl.ds(part * size, size)
        copies.append(
            fetch(
                [
                    (mat_hbm.at[some], mat.at[some]),
                    (e_hbm.at[:, some], e_in.at[:, some]),
                    (h_hbm.at[:, some], h_in.at[:, some]),
                ],
                sems.at[part],
            )
        )
    for copy in scalars:
        copy.wait()
    conduct = conductivity(peak[0], (SUB, depth)) * (0.5 * TIME_STEP)
    levels = []
    for index in range(NMAT):
        half = conduct / perm[index]
        levels.append(
            ((1.0 - half) / (1.0 + half), TIME_STEP / perm[index] / (1.0 + half))
        )

    def one_row(x, carry):
        for j in range(width // SUB):
            tile = pl.ds(SUB * j, SUB)
            level = mat[x, tile]
            retain, factor = levels[0]
            for index in range(1, NMAT):
                retain = jnp.where(level == index, levels[index][0], retain)
                factor = jnp.where(level == index, levels[index][1], factor)
            c_ref[0, x, tile] = retain
            c_ref[1, x, tile] = factor
        for m in range(6):
            e_ref[m, x] = e_in[m, x].astype(F32)
            h_ref[m, x] = h_in[m, x].astype(F32)
        return carry

    for part in range(parts):
        for copy in copies[part]:
            copy.wait()
        lax.fori_loop(part * size, (part + 1) * size, one_row, 0)


def conductivity(peak, shape):
    depth = shape[-1]
    height = lax.broadcasted_iota(jnp.int32, shape, len(shape) - 1).astype(F32)
    low = jnp.maximum(PML - height, 0.0) / PML
    high = jnp.maximum(height - (depth - 1 - PML), 0.0) / PML
    return peak * (low * low * low + high * high * high)


def inner_kernel(phase, step, p_ref, c_ref, sheet_ref, e_in, h_in, e_ref, h_ref):
    rows = e_ref.shape[1]
    middle = rows // 2
    cosine, sine, drive = p_ref[COS], p_ref[SIN], p_ref[DRIVE + step]
    keep, gain = p_ref[KEEP], p_ref[GAIN]
    upper = is_upper(phase)
    lo = jnp.where(upper, middle, 0)
    hi = jnp.where(upper, rows - 1, middle)
    skip = 1 if phase == 0 else jnp.where(upper, 0, 1)

    def new_h(x):
        h_row(e_ref, h_ref, x, keep, gain, cosine, sine)

    def new_electric(x):
        e_row(e_ref, h_ref, c_ref, sheet_ref, x, drive, cosine, sine)

    def start_row(x, carry):
        new_h(x)
        return carry

    def one_row(x, carry):
        new_h(x + 1)
        new_electric(x)
        return carry

    lax.fori_loop(lo, lo + skip + 1, start_row, 0)
    lax.fori_loop(lo + skip, hi - 1, one_row, 0)
    new_electric(hi - 1)

    @pl.when(upper)
    def _():
        ey, ez = (load_couple(e_ref, m, rows - 1) for m in (1, 2))
        hx = load_couple(h_ref, 0, rows - 1)
        store_couple(h_ref, new_hx(ey, ez, hx, keep, gain, cosine, sine), 0, rows - 1)

    if phase == 1:

        @pl.when(jnp.logical_not(upper))
        def _():
            new_electric(middle)


def edge_step(
    phase, step, p_ref, c_ref, sheet_ref, mine_ref, their_ref, e_ref, h_ref, out_ref=None
):
    cosine, sine, drive = p_ref[COS], p_ref[SIN], p_ref[DRIVE + step]
    keep, gain = p_ref[KEEP], p_ref[GAIN]
    top = e_ref.shape[1] - 1
    upper = is_upper(phase)

    @pl.when(upper)
    def _():
        part_y, part_z = (load_couple(mine_ref, m) for m in range(2))
        ey_above, ez_above = (
            turn(load_couple(their_ref, m), p_ref[END], p_ref[END + 1]) for m in range(2)
        )
        hy, hz = close_h(part_y, part_z, ey_above, ez_above, gain)
        store_couple(h_ref, hy, 1, top)
        store_couple(h_ref, hz, 2, top)
        ex, ey, ez = e_row(e_ref, h_ref, c_ref, sheet_ref, top, drive, cosine, sine)
        if out_ref is not None:
            part_y, part_z = partial_h(ex, ey, ez, hy, hz, keep, gain, cosine, sine)
            store_couple(out_ref, part_y, 0)
            store_couple(out_ref, part_z, 1)

    @pl.when(jnp.logical_not(upper))
    def _():
        part_y, part_z = (
            turn(load_couple(their_ref, m), p_ref[START], p_ref[START + 1])
            for m in range(2)
        )
        ey, ez = (load_couple(e_ref, m, 0) for m in (1, 2))
        below = close_h(part_y, part_z, ey, ez, gain)
        _, ey, ez = e_row(
            e_ref, h_ref, c_ref, sheet_ref, 0, drive, cosine, sine, below
        )
        if out_ref is not None:
            store_couple(out_ref, ey, 0)
            store_couple(out_ref, ez, 1)


def edge_kernel(
    phase, step, p_ref, c_ref, sheet_ref, mine_ref, their_ref, e_in, h_in,
    e_ref, h_ref, *out_ref,
):
    edge_step(
        phase, step, p_ref, c_ref, sheet_ref, mine_ref, their_ref, e_ref, h_ref, *out_ref
    )


def last_kernel(
    phase, step, slot, scale, p_ref, c_ref, sheet_ref, mine_ref, their_ref, old_ref,
    e_in, h_in, e_ref, h_ref, out_ref,
):
    edge_step(phase, step, p_ref, c_ref, sheet_ref, mine_ref, their_ref, e_ref, h_ref)
    total = jnp.zeros(old_ref.shape, F32)
    for x in (0, e_ref.shape[1] - 1):
        for m in range(4):
            for tile in load(e_ref, m, x):
                total = total + tile * tile
    out_ref[...] = old_ref[...] + monitor(total, slot, scale)


def monitor(total, slot, scale):
    lanes = lax.broadcasted_iota(jnp.int32, total.shape, 1)
    total = jnp.where(lanes == PML + 6, total, 0.0)
    total = jnp.sum(jnp.sum(total, 0, keepdims=True), 1, keepdims=True) * scale
    return jnp.where(lanes == slot, total, 0.0)


def power_kernel(phase, slot, scale, e_ref, old_ref, out_ref):
    rows, _, depth = e_ref.shape[1:]
    lo, hi = 1, rows - 1
    if phase is not None:
        middle, upper = rows // 2, is_upper(phase)
        lo = jnp.where(upper, middle + (1 - phase), 0)
        hi = jnp.where(upper, rows, middle + phase)

    def one_row(x, total):
        for m in range(4):
            for tile in load(e_ref, m, x):
                total = total + tile * tile
        return total

    total = lax.fori_loop(lo, hi, one_row, jnp.zeros((SUB, depth), F32))
    out_ref[...] = old_ref[...] + monitor(total, slot, scale)


def move(pairs, sems):
    for copy in fetch(pairs, sems):
        copy.wait()


def inner_out_kernel(e_ref, h_ref, e_out, h_out, sems):
    rows = e_ref.shape[1]
    some, most = pl.ds(1, rows - 2), pl.ds(0, rows - 1)
    move(
        [(e_ref.at[:, some], e_out.at[:, some]), (h_ref.at[:, most], h_out.at[:, most])],
        sems,
    )


def edge_out_kernel(e_ref, h_ref, e_in, h_in, e_out, h_out, sems):
    end = e_ref.shape[1] - 1
    move(
        [
            (e_ref.at[:, 0], e_out.at[:, 0]),
            (e_ref.at[:, end], e_out.at[:, end]),
            (h_ref.at[:, end], h_out.at[:, end]),
        ],
        sems,
    )


def add_kernel(scale, *refs):
    total = refs[0][...]
    for ref in refs[1:-1]:
        total = total + ref[...]
    refs[-1][...] = total * scale if scale != 1.0 else total


def call(kernel, outs, ins, specs, aliases=None, scratch=(), flops=0, vmem=16):
    return pl.pallas_call(
        kernel,
        out_shape=tuple(pltpu.VMEM(shape, F32) for shape in outs),
        in_specs=specs,
        out_specs=tuple(VMEM for _ in outs),
        input_output_aliases=aliases or {},
        scratch_shapes=scratch,
        cost_estimate=pl.CostEstimate(flops=flops, bytes_accessed=0, transcendentals=0),
        compiler_params=pltpu.CompilerParams(vmem_limit_bytes=vmem * 2**20),
    )(*ins)


def swap(value, phase):
    count = lax.axis_size("sp")
    pairs = [(i, (((i - phase) % count ^ 1) + phase) % count) for i in range(count)]
    return lax.ppermute(value, "sp", pairs)


def shift(value, axis, steps):
    count = lax.axis_size(axis)
    return lax.ppermute(value, axis, [(i, (i + steps) % count) for i in range(count)])


def total_over(value, axis, scale=1.0):
    count = lax.axis_size(axis)
    shape = value.shape
    if count & (count - 1):
        parts = [value] + [shift(value, axis, step) for step in range(1, count)]
        return call(functools.partial(add_kernel, scale), [shape], parts, [VMEM] * count)[0]
    step = 1
    while step < count:
        other = lax.ppermute(value, axis, [(i, i ^ step) for i in range(count)])
        step *= 2
        last = scale if step >= count else 1.0
        value = call(
            functools.partial(add_kernel, last), [shape], [value, other], [VMEM] * 2
        )[0]
    return value


def to_hbm(kernel, shape, ins, specs, copies, aliases=None):
    whole = jax.ShapeDtypeStruct(shape, F32)
    return pl.pallas_call(
        kernel,
        out_shape=(whole, whole),
        in_specs=specs,
        out_specs=(HBM, HBM),
        input_output_aliases=aliases or {},
        scratch_shapes=[pltpu.SemaphoreType.DMA((copies,))],
        compiler_params=pltpu.CompilerParams(vmem_limit_bytes=2**20),
    )(*ins)


def on_device(
    bloch_index,
    material,
    permittivity,
    absorption_peak,
    source_sheet,
    waveform,
    electric_in,
    magnetic_in,
):
    points = bloch_index.shape[0]
    rows, width, depth = material.shape
    total_points = points * lax.axis_size("ka")
    cells_plane = rows * lax.axis_size("sp") * width
    plane = (jnp.arange(depth) == PML + 2).astype(F32)
    sheets = source_sheet[..., None] * plane
    results = [
        one_point(
            bloch_index[point : point + 1], sheets[point], waveform, material, permittivity,
            absorption_peak, electric_in[point], magnetic_in[point], 1.0 / cells_plane,
        )
        for point in range(points)
    ]
    electric, magnetic, powers = zip(*results)
    sums = [total_over(power, "sp") for power in powers]
    local = sums[0]
    for other in sums[1:]:
        local = local + other
    mean = total_over(local, "ka", 1.0 / total_points)
    return (
        jnp.stack(electric),
        jnp.stack(magnetic),
        jnp.stack([total[0, :NSNAP] for total in sums]),
        mean[0, :NSNAP],
    )


def one_point(
    bloch, sheet, waveform, material, permittivity, peak, electric_in, magnetic_in, scale
):
    rows, width, depth = material.shape
    steps = waveform.shape[0]
    edge = (4, width, depth)
    full = (6, rows, width, depth)
    dtype = electric_in.dtype
    electric_in, magnetic_in, material = (
        pltpu.with_memory_space_constraint(value, pltpu.HBM)
        for value in (electric_in, magnetic_in, material)
    )
    p, *mine = call(
        first_kernel,
        [(DRIVE + steps, SUB, depth), edge, edge],
        [bloch, peak, waveform, electric_in, magnetic_in],
        [ANY] * 3 + [HBM] * 2,
        scratch=[
            pltpu.SMEM(bloch.shape, bloch.dtype),
            pltpu.SMEM(peak.shape, F32),
            pltpu.SMEM(waveform.shape, F32),
            pltpu.VMEM((4, width, depth), dtype),
            pltpu.VMEM((6, width, depth), dtype),
            pltpu.VMEM((4, width, depth), dtype),
            pltpu.SemaphoreType.DMA((6,)),
        ],
    )
    their = [swap(mine[phase], phase) for phase in range(2)]
    e, h, c = call(
        widen_kernel,
        [full, full, (2, rows, width, depth)],
        [peak, permittivity, material, electric_in, magnetic_in],
        [ANY] * 2 + [HBM] * 3,
        scratch=[
            pltpu.SMEM(peak.shape, F32),
            pltpu.SMEM(permittivity.shape, F32),
            pltpu.VMEM(material.shape, material.dtype),
            pltpu.VMEM(full, dtype),
            pltpu.VMEM(full, dtype),
            pltpu.SemaphoreType.DMA((2,)),
            pltpu.SemaphoreType.DMA((4, 3)),
        ],
    )
    power = jnp.zeros((SUB, depth), F32)

    def inner(phase, step, e, h):
        return call(
            functools.partial(inner_kernel, phase, step),
            [full, full],
            [p, c, sheet, e, h],
            [VMEM] * 5,
            {3: 0, 4: 1},
        )

    def measured(phase, step, power, e):
        return call(
            functools.partial(power_kernel, phase, step // INTERVAL, scale),
            [(SUB, depth)],
            [e, power],
            [VMEM, VMEM],
        )[0]

    for phase in range(2):
        e, h = inner(phase, 0, e, h)
    for step in range(steps - 1):
        for phase in range(2):
            e, h, mine[phase] = call(
                functools.partial(edge_kernel, phase, step),
                [full, full, edge],
                [p, c, sheet, mine[phase], their[phase], e, h],
                [VMEM] * 7,
                {5: 0, 6: 1},
            )
            if (step + 1) % INTERVAL == 0:
                power = measured(phase, step, power, e)
            their[phase] = swap(mine[phase], phase)
            e, h = inner(phase, step + 1, e, h)
    step = steps - 1
    power = measured(None, step, power, e)
    e_out, h_out = to_hbm(inner_out_kernel, full, [e, h], [VMEM, VMEM], 2)
    e, h = call(
        functools.partial(edge_kernel, 0, step),
        [full, full],
        [p, c, sheet, mine[0], their[0], e, h],
        [VMEM] * 7,
        {5: 0, 6: 1},
    )
    e, h, power = call(
        functools.partial(last_kernel, 1, step, step // INTERVAL, scale),
        [full, full, (SUB, depth)],
        [p, c, sheet, mine[1], their[1], power, e, h],
        [VMEM] * 8,
        {6: 0, 7: 1},
    )
    e_out, h_out = to_hbm(
        edge_out_kernel, full, [e, h, e_out, h_out], [VMEM, VMEM, HBM, HBM], 3, {2: 0, 3: 1}
    )
    return e_out, h_out, power


def solution(mesh):
    in_specs = (
        P("ka", None),
        P("sp", None, None),
        P(),
        P(),
        P("ka", None, "sp", None),
        P(),
        P("ka", None, "sp", None, None),
        P("ka", None, "sp", None, None),
    )
    out_specs = (
        P("ka", None, "sp", None, None),
        P("ka", None, "sp", None, None),
        P("ka", None),
        P(),
    )
    return jax.shard_map(
        on_device, mesh=mesh, in_specs=in_specs, out_specs=out_specs, check_vma=False
    )
```

```python
import functools

import jax
import jax.numpy as jnp
from jax import lax
from jax.experimental import pallas as pl
from jax.experimental.pallas import tpu as pltpu
from jax.sharding import PartitionSpec as P


PML = 16
INTERVAL = 5
NSNAP = 2
MPHASE = 64
NMAT = 3
TIME_STEP = 0.5
SUB = 8

VMEM = pl.BlockSpec(memory_space=pltpu.VMEM)
SMEM = pl.BlockSpec(memory_space=pltpu.SMEM)
HBM = pl.BlockSpec(memory_space=pltpu.HBM)
ANY = pl.BlockSpec(memory_space=pl.ANY)
F32 = jnp.float32

COS, SIN, END, START, KEEP, GAIN, DRIVE = 0, 1, 2, 4, 6, 7, 8


def load(ref, *where):
    tiles = ref.shape[-2] // SUB
    return [ref[(*where, pl.ds(SUB * j, SUB))].astype(F32) for j in range(tiles)]


def load_couple(ref, member, *where):
    return (load(ref, 2 * member, *where), load(ref, 2 * member + 1, *where))


def store(ref, values, *where):
    for j, tile in enumerate(values):
        ref[(*where, pl.ds(SUB * j, SUB))] = tile


def store_couple(ref, couple, member, *where):
    store(ref, couple[0], 2 * member, *where)
    store(ref, couple[1], 2 * member + 1, *where)


def both(fn, *couples):
    return tuple(
        [fn(*tiles) for tiles in zip(*parts)] for parts in zip(*couples)
    )


def scaled(planes, fn, couple, *others):
    out = []
    for part in range(2):
        parts = [couple[part], *(other[part] for other in others)]
        out.append([fn(*tiles) for tiles in zip(*planes, *parts)])
    return tuple(out)


def turn(couple, cosine, sine):
    return (
        [re * cosine - im * sine for re, im in zip(*couple)],
        [re * sine + im * cosine for re, im in zip(*couple)],
    )


def next_y(couple, cosine, sine):
    rows = lax.broadcasted_iota(jnp.int32, couple[0][0].shape, 0)
    wrapped = turn((couple[0][:1], couple[1][:1]), cosine, sine)
    out = []
    for part, edge in zip(couple, wrapped):
        after = part[1:] + edge
        out.append(
            [
                pltpu.roll(jnp.where(rows == 0, there, here), SUB - 1, 0)
                for here, there in zip(part, after)
            ]
        )
    return tuple(out)


def prior_y(couple, cosine, sine):
    rows = lax.broadcasted_iota(jnp.int32, couple[0][0].shape, 0)
    wrapped = turn((couple[0][-1:], couple[1][-1:]), cosine, -sine)
    out = []
    for part, edge in zip(couple, wrapped):
        before = edge + part[:-1]
        out.append(
            [
                pltpu.roll(jnp.where(rows == SUB - 1, there, here), 1, 0)
                for here, there in zip(part, before)
            ]
        )
    return tuple(out)


def next_z(couple):
    depth = couple[0][0].shape[1]
    lanes = lax.broadcasted_iota(jnp.int32, couple[0][0].shape, 1)
    return both(
        lambda tile: jnp.where(lanes == depth - 1, 0.0, pltpu.roll(tile, depth - 1, 1)),
        couple,
    )


def prior_z(couple):
    lanes = lax.broadcasted_iota(jnp.int32, couple[0][0].shape, 1)
    return both(lambda tile: jnp.where(lanes == 0, 0.0, pltpu.roll(tile, 1, 1)), couple)


def new_hx(ey, ez, hx, keep, gain, cosine, sine):
    return both(
        lambda h, z_up, z, y_up, y: keep * h + gain * ((z_up - z) - (y_up - y)),
        hx,
        next_y(ez, cosine, sine),
        ez,
        next_z(ey),
        ey,
    )


def partial_h(ex, ey, ez, hy, hz, keep, gain, cosine, sine):
    part_y = both(
        lambda h, x_up, x, z: keep * h + gain * ((x_up - x) + z), hy, next_z(ex), ex, ez
    )
    part_z = both(
        lambda h, x_up, x, y: keep * h - gain * ((x_up - x) + y),
        hz,
        next_y(ex, cosine, sine),
        ex,
        ey,
    )
    return part_y, part_z


def close_h(part_y, part_z, ey_above, ez_above, gain):
    return (
        both(lambda h, z: h - gain * z, part_y, ez_above),
        both(lambda h, y: h + gain * y, part_z, ey_above),
    )


def h_row(e_ref, h_ref, x, keep, gain, cosine, sine):
    ex, ey, ez = (load_couple(e_ref, m, x) for m in range(3))
    ey_above, ez_above = (load_couple(e_ref, m, x + 1) for m in (1, 2))
    hx, hy, hz = (load_couple(h_ref, m, x) for m in range(3))
    new_x = new_hx(ey, ez, hx, keep, gain, cosine, sine)
    new_y = both(
        lambda h, x_up, x_, z_up, z: keep * h + gain * ((x_up - x_) - (z_up - z)),
        hy,
        next_z(ex),
        ex,
        ez_above,
        ez,
    )
    new_z = both(
        lambda h, y_up, y, x_up, x_: keep * h + gain * ((y_up - y) - (x_up - x_)),
        hz,
        ey_above,
        ey,
        next_y(ex, cosine, sine),
        ex,
    )
    store_couple(h_ref, new_x, 0, x)
    store_couple(h_ref, new_y, 1, x)
    store_couple(h_ref, new_z, 2, x)


def new_e(e, h, hy_below, hz_below, retain, factor, sheet, drive, cosine, sine):
    ex, ey, ez = e
    hx, hy, hz = h
    drive_x = both(lambda s: drive * s, sheet)
    new_x = scaled(
        (retain, factor),
        lambda r, f, e_, z, z_dn, y, y_dn, s: r * e_ + f * ((z - z_dn) - (y - y_dn) - s),
        ex,
        hz,
        prior_y(hz, cosine, sine),
        hy,
        prior_z(hy),
        drive_x,
    )
    new_y = scaled(
        (retain, factor),
        lambda r, f, e_, x, x_dn, z, z_dn: r * e_ + f * ((x - x_dn) - (z - z_dn)),
        ey,
        hx,
        prior_z(hx),
        hz,
        hz_below,
    )
    new_z = scaled(
        (retain, factor),
        lambda r, f, e_, y, y_dn, x, x_dn: r * e_ + f * ((y - y_dn) - (x - x_dn)),
        ez,
        hy,
        hy_below,
        hx,
        prior_y(hx, cosine, sine),
    )
    return new_x, new_y, new_z


def e_row(e_ref, h_ref, c_ref, sheet_ref, x, drive, cosine, sine, below=None):
    e = [load_couple(e_ref, m, x) for m in range(3)]
    h = [load_couple(h_ref, m, x) for m in range(3)]
    if below is None:
        below = [load_couple(h_ref, m, x - 1) for m in (1, 2)]
    retain, factor = load(c_ref, 0, x), load(c_ref, 1, x)
    sheet = (load(sheet_ref, 0, x), load(sheet_ref, 1, x))
    new = new_e(e, h, *below, retain, factor, sheet, drive, cosine, sine)
    for m in range(3):
        store_couple(e_ref, new[m], m, x)
    return new


def is_upper(phase):
    return lax.axis_index("sp") % 2 == phase


def fetch(pairs, sems):
    copies = [
        pltpu.make_async_copy(source, target, sems.at[i])
        for i, (source, target) in enumerate(pairs)
    ]
    for copy in copies:
        copy.start()
    return copies


def first_kernel(
    bloch_hbm, peak_hbm, wave_hbm, e_hbm, h_hbm, p_ref, one_ref, two_ref,
    bloch, peak, wave, low, high, mag, sems,
):
    rows = e_hbm.shape[1]
    copies = fetch(
        [
            (bloch_hbm, bloch),
            (peak_hbm, peak),
            (wave_hbm, wave),
            (e_hbm.at[pl.ds(2, 4), 0], low),
            (e_hbm.at[:, rows - 1], high),
            (h_hbm.at[pl.ds(2, 4), rows - 1], mag),
        ],
        sems,
    )
    for copy in copies[:3]:
        copy.wait()
    shape = p_ref.shape[1:]
    angle_x, angle_y = (
        2.0 * jnp.pi * jnp.full(shape, bloch[0, axis].astype(F32)) / MPHASE
        for axis in range(2)
    )
    cos_x, sin_x = jnp.cos(angle_x), jnp.sin(angle_x)
    slab, slabs = lax.axis_index("sp"), lax.axis_size("sp")
    at_end, at_start = slab == slabs - 1, slab == 0
    half = conductivity(peak[0], shape) * (0.5 * TIME_STEP)
    p_ref[COS] = cosine = jnp.cos(angle_y)
    p_ref[SIN] = sine = jnp.sin(angle_y)
    p_ref[END] = jnp.where(at_end, cos_x, 1.0)
    p_ref[END + 1] = jnp.where(at_end, sin_x, 0.0)
    p_ref[START] = jnp.where(at_start, cos_x, 1.0)
    p_ref[START + 1] = jnp.where(at_start, -sin_x, 0.0)
    p_ref[KEEP] = keep = (1.0 - half) / (1.0 + half)
    p_ref[GAIN] = gain = -TIME_STEP / (1.0 + half)
    for step in range(wave.shape[0]):
        p_ref[DRIVE + step] = jnp.full(shape, wave[step])
    for copy in copies[3:]:
        copy.wait()

    def write(d_ref, s_ref):
        d_ref[...] = low[...].astype(F32)
        ex, ey, ez = (load_couple(high, m) for m in range(3))
        hy, hz = (load_couple(mag, m) for m in range(2))
        part_y, part_z = partial_h(ex, ey, ez, hy, hz, keep, gain, cosine, sine)
        store_couple(s_ref, part_y, 0)
        store_couple(s_ref, part_z, 1)

    @pl.when(is_upper(0))
    def _():
        write(two_ref, one_ref)

    @pl.when(jnp.logical_not(is_upper(0)))
    def _():
        write(one_ref, two_ref)


def widen_kernel(
    peak_hbm, perm_hbm, mat_hbm, e_hbm, h_hbm, e_ref, h_ref, c_ref,
    peak, perm, mat, e_in, h_in, small, sems,
):
    rows, width, depth = mat.shape
    parts = sems.shape[0]
    size = rows // parts
    scalars = fetch([(peak_hbm, peak), (perm_hbm, perm)], small)
    copies = []
    for part in range(parts):
        some = pl.ds(part * size, size)
        copies.append(
            fetch(
                [
                    (mat_hbm.at[some], mat.at[some]),
                    (e_hbm.at[:, some], e_in.at[:, some]),
                    (h_hbm.at[:, some], h_in.at[:, some]),
                ],
                sems.at[part],
            )
        )
    for copy in scalars:
        copy.wait()
    conduct = conductivity(peak[0], (SUB, depth)) * (0.5 * TIME_STEP)
    levels = []
    for index in range(NMAT):
        half = conduct / perm[index]
        levels.append(
            ((1.0 - half) / (1.0 + half), TIME_STEP / perm[index] / (1.0 + half))
        )

    def one_row(x, carry):
        for j in range(width // SUB):
            tile = pl.ds(SUB * j, SUB)
            level = mat[x, tile]
            retain, factor = levels[0]
            for index in range(1, NMAT):
                retain = jnp.where(level == index, levels[index][0], retain)
                factor = jnp.where(level == index, levels[index][1], factor)
            c_ref[0, x, tile] = retain
            c_ref[1, x, tile] = factor
        for m in range(6):
            e_ref[m, x] = e_in[m, x].astype(F32)
            h_ref[m, x] = h_in[m, x].astype(F32)
        return carry

    for part in range(parts):
        for copy in copies[part]:
            copy.wait()
        lax.fori_loop(part * size, (part + 1) * size, one_row, 0)


def conductivity(peak, shape):
    depth = shape[-1]
    height = lax.broadcasted_iota(jnp.int32, shape, len(shape) - 1).astype(F32)
    low = jnp.maximum(PML - height, 0.0) / PML
    high = jnp.maximum(height - (depth - 1 - PML), 0.0) / PML
    return peak * (low * low * low + high * high * high)


def inner_kernel(phase, step, p_ref, c_ref, sheet_ref, e_in, h_in, e_ref, h_ref):
    rows = e_ref.shape[1]
    middle = rows // 2
    cosine, sine, drive = p_ref[COS], p_ref[SIN], p_ref[DRIVE + step]
    keep, gain = p_ref[KEEP], p_ref[GAIN]
    upper = is_upper(phase)
    lo = jnp.where(upper, middle, 0)
    hi = jnp.where(upper, rows - 1, middle)
    skip = 1 if phase == 0 else jnp.where(upper, 0, 1)

    def new_h(x):
        h_row(e_ref, h_ref, x, keep, gain, cosine, sine)

    def new_electric(x):
        e_row(e_ref, h_ref, c_ref, sheet_ref, x, drive, cosine, sine)

    def start_row(x, carry):
        new_h(x)
        return carry

    def one_row(x, carry):
        new_h(x + 1)
        new_electric(x)
        return carry

    lax.fori_loop(lo, lo + skip + 1, start_row, 0)
    lax.fori_loop(lo + skip, hi - 1, one_row, 0)
    new_electric(hi - 1)

    @pl.when(upper)
    def _():
        ey, ez = (load_couple(e_ref, m, rows - 1) for m in (1, 2))
        hx = load_couple(h_ref, 0, rows - 1)
        store_couple(h_ref, new_hx(ey, ez, hx, keep, gain, cosine, sine), 0, rows - 1)

    if phase == 1:

        @pl.when(jnp.logical_not(upper))
        def _():
            new_electric(middle)


def edge_step(
    phase, step, p_ref, c_ref, sheet_ref, mine_ref, their_ref, e_ref, h_ref, out_ref=None
):
    cosine, sine, drive = p_ref[COS], p_ref[SIN], p_ref[DRIVE + step]
    keep, gain = p_ref[KEEP], p_ref[GAIN]
    top = e_ref.shape[1] - 1
    upper = is_upper(phase)

    @pl.when(upper)
    def _():
        part_y, part_z = (load_couple(mine_ref, m) for m in range(2))
        ey_above, ez_above = (
            turn(load_couple(their_ref, m), p_ref[END], p_ref[END + 1]) for m in range(2)
        )
        hy, hz = close_h(part_y, part_z, ey_above, ez_above, gain)
        store_couple(h_ref, hy, 1, top)
        store_couple(h_ref, hz, 2, top)
        ex, ey, ez = e_row(e_ref, h_ref, c_ref, sheet_ref, top, drive, cosine, sine)
        if out_ref is not None:
            part_y, part_z = partial_h(ex, ey, ez, hy, hz, keep, gain, cosine, sine)
            store_couple(out_ref, part_y, 0)
            store_couple(out_ref, part_z, 1)

    @pl.when(jnp.logical_not(upper))
    def _():
        part_y, part_z = (
            turn(load_couple(their_ref, m), p_ref[START], p_ref[START + 1])
            for m in range(2)
        )
        ey, ez = (load_couple(e_ref, m, 0) for m in (1, 2))
        below = close_h(part_y, part_z, ey, ez, gain)
        _, ey, ez = e_row(
            e_ref, h_ref, c_ref, sheet_ref, 0, drive, cosine, sine, below
        )
        if out_ref is not None:
            store_couple(out_ref, ey, 0)
            store_couple(out_ref, ez, 1)


def edge_kernel(
    phase, step, p_ref, c_ref, sheet_ref, mine_ref, their_ref, e_in, h_in,
    e_ref, h_ref, *out_ref,
):
    edge_step(
        phase, step, p_ref, c_ref, sheet_ref, mine_ref, their_ref, e_ref, h_ref, *out_ref
    )


def last_kernel(
    phase, step, slot, scale, p_ref, c_ref, sheet_ref, mine_ref, their_ref, old_ref,
    e_in, h_in, e_ref, h_ref, out_ref,
):
    edge_step(phase, step, p_ref, c_ref, sheet_ref, mine_ref, their_ref, e_ref, h_ref)
    total = jnp.zeros(old_ref.shape, F32)
    for x in (0, e_ref.shape[1] - 1):
        for m in range(4):
            for tile in load(e_ref, m, x):
                total = total + tile * tile
    out_ref[...] = old_ref[...] + monitor(total, slot, scale)


def monitor(total, slot, scale):
    lanes = lax.broadcasted_iota(jnp.int32, total.shape, 1)
    total = jnp.where(lanes == PML + 6, total, 0.0)
    total = jnp.sum(jnp.sum(total, 0, keepdims=True), 1, keepdims=True) * scale
    return jnp.where(lanes == slot, total, 0.0)


def power_kernel(phase, slot, scale, e_ref, old_ref, out_ref):
    rows, _, depth = e_ref.shape[1:]
    lo, hi = 1, rows - 1
    if phase is not None:
        middle, upper = rows // 2, is_upper(phase)
        lo = jnp.where(upper, middle + (1 - phase), 0)
        hi = jnp.where(upper, rows, middle + phase)

    def one_row(x, total):
        for m in range(4):
            for tile in load(e_ref, m, x):
                total = total + tile * tile
        return total

    total = lax.fori_loop(lo, hi, one_row, jnp.zeros((SUB, depth), F32))
    out_ref[...] = old_ref[...] + monitor(total, slot, scale)


def out_kernel(in_ref, out_ref, sems):
    for copy in fetch([(in_ref, out_ref)], sems):
        copy.wait()


def add_kernel(scale, *refs):
    total = refs[0][...]
    for ref in refs[1:-1]:
        total = total + ref[...]
    refs[-1][...] = total * scale if scale != 1.0 else total


def call(kernel, outs, ins, specs, aliases=None, scratch=(), flops=0, vmem=16):
    return pl.pallas_call(
        kernel,
        out_shape=tuple(pltpu.VMEM(shape, F32) for shape in outs),
        in_specs=specs,
        out_specs=tuple(VMEM for _ in outs),
        input_output_aliases=aliases or {},
        scratch_shapes=scratch,
        cost_estimate=pl.CostEstimate(flops=flops, bytes_accessed=0, transcendentals=0),
        compiler_params=pltpu.CompilerParams(vmem_limit_bytes=vmem * 2**20),
    )(*ins)


def swap(value, phase):
    count = lax.axis_size("sp")
    pairs = [(i, (((i - phase) % count ^ 1) + phase) % count) for i in range(count)]
    return lax.ppermute(value, "sp", pairs)


def shift(value, axis, steps):
    count = lax.axis_size(axis)
    return lax.ppermute(value, axis, [(i, (i + steps) % count) for i in range(count)])


def total_over(value, axis, scale=1.0):
    count = lax.axis_size(axis)
    shape = value.shape
    if count & (count - 1):
        parts = [value] + [shift(value, axis, step) for step in range(1, count)]
        return call(functools.partial(add_kernel, scale), [shape], parts, [VMEM] * count)[0]
    step = 1
    while step < count:
        other = lax.ppermute(value, axis, [(i, i ^ step) for i in range(count)])
        step *= 2
        last = scale if step >= count else 1.0
        value = call(
            functools.partial(add_kernel, last), [shape], [value, other], [VMEM] * 2
        )[0]
    return value


def to_hbm(value):
    return pl.pallas_call(
        out_kernel,
        out_shape=jax.ShapeDtypeStruct(value.shape, F32),
        in_specs=[VMEM],
        out_specs=HBM,
        scratch_shapes=[pltpu.SemaphoreType.DMA((1,))],
        compiler_params=pltpu.CompilerParams(vmem_limit_bytes=2**20),
    )(value)


def on_device(
    bloch_index,
    material,
    permittivity,
    absorption_peak,
    source_sheet,
    waveform,
    electric_in,
    magnetic_in,
):
    points = bloch_index.shape[0]
    rows, width, depth = material.shape
    total_points = points * lax.axis_size("ka")
    cells_plane = rows * lax.axis_size("sp") * width
    plane = (jnp.arange(depth) == PML + 2).astype(F32)
    sheets = source_sheet[..., None] * plane
    results = [
        one_point(
            bloch_index[point : point + 1], sheets[point], waveform, material, permittivity,
            absorption_peak, electric_in[point], magnetic_in[point], 1.0 / cells_plane,
        )
        for point in range(points)
    ]
    electric, magnetic, powers = zip(*results)
    sums = [total_over(power, "sp") for power in powers]
    electric = [to_hbm(value) for value in electric]
    local = sums[0]
    for other in sums[1:]:
        local = local + other
    mean = total_over(local, "ka", 1.0 / total_points)
    magnetic = [to_hbm(value) for value in magnetic]
    return (
        jnp.stack(electric),
        jnp.stack(magnetic),
        jnp.stack([total[0, :NSNAP] for total in sums]),
        mean[0, :NSNAP],
    )


def one_point(
    bloch, sheet, waveform, material, permittivity, peak, electric_in, magnetic_in, scale
):
    rows, width, depth = material.shape
    steps = waveform.shape[0]
    edge = (4, width, depth)
    full = (6, rows, width, depth)
    dtype = electric_in.dtype
    bloch, waveform, permittivity, electric_in, magnetic_in, material = (
        pltpu.with_memory_space_constraint(value, pltpu.HBM)
        for value in (bloch, waveform, permittivity, electric_in, magnetic_in, material)
    )
    p, *mine = call(
        first_kernel,
        [(DRIVE + steps, SUB, depth), edge, edge],
        [bloch, peak, waveform, electric_in, magnetic_in],
        [HBM, ANY] + [HBM] * 3,
        scratch=[
            pltpu.SMEM(bloch.shape, bloch.dtype),
            pltpu.SMEM(peak.shape, F32),
            pltpu.SMEM(waveform.shape, F32),
            pltpu.VMEM((4, width, depth), dtype),
            pltpu.VMEM((6, width, depth), dtype),
            pltpu.VMEM((4, width, depth), dtype),
            pltpu.SemaphoreType.DMA((6,)),
        ],
    )
    their = [swap(mine[phase], phase) for phase in range(2)]
    e, h, c = call(
        widen_kernel,
        [full, full, (2, rows, width, depth)],
        [peak, permittivity, material, electric_in, magnetic_in],
        [ANY] + [HBM] * 4,
        scratch=[
            pltpu.SMEM(peak.shape, F32),
            pltpu.SMEM(permittivity.shape, F32),
            pltpu.VMEM(material.shape, material.dtype),
            pltpu.VMEM(full, dtype),
            pltpu.VMEM(full, dtype),
            pltpu.SemaphoreType.DMA((2,)),
            pltpu.SemaphoreType.DMA((4, 3)),
        ],
    )
    power = jnp.zeros((SUB, depth), F32)

    def inner(phase, step, e, h):
        return call(
            functools.partial(inner_kernel, phase, step),
            [full, full],
            [p, c, sheet, e, h],
            [VMEM] * 5,
            {3: 0, 4: 1},
        )

    def measured(phase, step, power, e):
        return call(
            functools.partial(power_kernel, phase, step // INTERVAL, scale),
            [(SUB, depth)],
            [e, power],
            [VMEM, VMEM],
        )[0]

    for phase in range(2):
        e, h = inner(phase, 0, e, h)
    for step in range(steps - 1):
        for phase in range(2):
            e, h, mine[phase] = call(
                functools.partial(edge_kernel, phase, step),
                [full, full, edge],
                [p, c, sheet, mine[phase], their[phase], e, h],
                [VMEM] * 7,
                {5: 0, 6: 1},
            )
            if (step + 1) % INTERVAL == 0:
                power = measured(phase, step, power, e)
            their[phase] = swap(mine[phase], phase)
            e, h = inner(phase, step + 1, e, h)
    step = steps - 1
    power = measured(None, step, power, e)
    e, h = call(
        functools.partial(edge_kernel, 0, step),
        [full, full],
        [p, c, sheet, mine[0], their[0], e, h],
        [VMEM] * 7,
        {5: 0, 6: 1},
    )
    e, h, power = call(
        functools.partial(last_kernel, 1, step, step // INTERVAL, scale),
        [full, full, (SUB, depth)],
        [p, c, sheet, mine[1], their[1], power, e, h],
        [VMEM] * 8,
        {6: 0, 7: 1},
    )
    return e, h, power


def solution(mesh):
    in_specs = (
        P("ka", None),
        P("sp", None, None),
        P(),
        P(),
        P("ka", None, "sp", None),
        P(),
        P("ka", None, "sp", None, None),
        P("ka", None, "sp", None, None),
    )
    out_specs = (
        P("ka", None, "sp", None, None),
        P("ka", None, "sp", None, None),
        P("ka", None),
        P(),
    )
    return jax.shard_map(
        on_device, mesh=mesh, in_specs=in_specs, out_specs=out_specs, check_vma=False
    )
```

```python
import functools

import jax
import jax.numpy as jnp
from jax import lax
from jax.experimental import pallas as pl
from jax.experimental.pallas import tpu as pltpu
from jax.sharding import PartitionSpec as P


PML = 16
INTERVAL = 5
NSNAP = 2
MPHASE = 64
NMAT = 3
TIME_STEP = 0.5
SUB = 8

VMEM = pl.BlockSpec(memory_space=pltpu.VMEM)
SMEM = pl.BlockSpec(memory_space=pltpu.SMEM)
HBM = pl.BlockSpec(memory_space=pltpu.HBM)
ANY = pl.BlockSpec(memory_space=pl.ANY)
F32 = jnp.float32

COS, SIN, END, START, KEEP, GAIN, DRIVE = 0, 1, 2, 4, 6, 7, 8


def load(ref, *where):
    tiles = ref.shape[-2] // SUB
    return [ref[(*where, pl.ds(SUB * j, SUB))].astype(F32) for j in range(tiles)]


def load_couple(ref, member, *where):
    return (load(ref, 2 * member, *where), load(ref, 2 * member + 1, *where))


def store(ref, values, *where):
    for j, tile in enumerate(values):
        ref[(*where, pl.ds(SUB * j, SUB))] = tile


def store_couple(ref, couple, member, *where):
    store(ref, couple[0], 2 * member, *where)
    store(ref, couple[1], 2 * member + 1, *where)


def both(fn, *couples):
    return tuple(
        [fn(*tiles) for tiles in zip(*parts)] for parts in zip(*couples)
    )


def scaled(planes, fn, couple, *others):
    out = []
    for part in range(2):
        parts = [couple[part], *(other[part] for other in others)]
        out.append([fn(*tiles) for tiles in zip(*planes, *parts)])
    return tuple(out)


def turn(couple, cosine, sine):
    return (
        [re * cosine - im * sine for re, im in zip(*couple)],
        [re * sine + im * cosine for re, im in zip(*couple)],
    )


def next_y(couple, cosine, sine):
    rows = lax.broadcasted_iota(jnp.int32, couple[0][0].shape, 0)
    wrapped = turn((couple[0][:1], couple[1][:1]), cosine, sine)
    out = []
    for part, edge in zip(couple, wrapped):
        after = part[1:] + edge
        out.append(
            [
                pltpu.roll(jnp.where(rows == 0, there, here), SUB - 1, 0)
                for here, there in zip(part, after)
            ]
        )
    return tuple(out)


def prior_y(couple, cosine, sine):
    rows = lax.broadcasted_iota(jnp.int32, couple[0][0].shape, 0)
    wrapped = turn((couple[0][-1:], couple[1][-1:]), cosine, -sine)
    out = []
    for part, edge in zip(couple, wrapped):
        before = edge + part[:-1]
        out.append(
            [
                pltpu.roll(jnp.where(rows == SUB - 1, there, here), 1, 0)
                for here, there in zip(part, before)
            ]
        )
    return tuple(out)


def next_z(couple):
    depth = couple[0][0].shape[1]
    lanes = lax.broadcasted_iota(jnp.int32, couple[0][0].shape, 1)
    return both(
        lambda tile: jnp.where(lanes == depth - 1, 0.0, pltpu.roll(tile, depth - 1, 1)),
        couple,
    )


def prior_z(couple):
    lanes = lax.broadcasted_iota(jnp.int32, couple[0][0].shape, 1)
    return both(lambda tile: jnp.where(lanes == 0, 0.0, pltpu.roll(tile, 1, 1)), couple)


def new_hx(ey, ez, hx, keep, gain, cosine, sine):
    return both(
        lambda h, z_up, z, y_up, y: keep * h + gain * ((z_up - z) - (y_up - y)),
        hx,
        next_y(ez, cosine, sine),
        ez,
        next_z(ey),
        ey,
    )


def partial_h(ex, ey, ez, hy, hz, keep, gain, cosine, sine):
    part_y = both(
        lambda h, x_up, x, z: keep * h + gain * ((x_up - x) + z), hy, next_z(ex), ex, ez
    )
    part_z = both(
        lambda h, x_up, x, y: keep * h - gain * ((x_up - x) + y),
        hz,
        next_y(ex, cosine, sine),
        ex,
        ey,
    )
    return part_y, part_z


def close_h(part_y, part_z, ey_above, ez_above, gain):
    return (
        both(lambda h, z: h - gain * z, part_y, ez_above),
        both(lambda h, y: h + gain * y, part_z, ey_above),
    )


def h_row(e_ref, h_ref, x, keep, gain, cosine, sine):
    ex, ey, ez = (load_couple(e_ref, m, x) for m in range(3))
    ey_above, ez_above = (load_couple(e_ref, m, x + 1) for m in (1, 2))
    hx, hy, hz = (load_couple(h_ref, m, x) for m in range(3))
    new_x = new_hx(ey, ez, hx, keep, gain, cosine, sine)
    new_y = both(
        lambda h, x_up, x_, z_up, z: keep * h + gain * ((x_up - x_) - (z_up - z)),
        hy,
        next_z(ex),
        ex,
        ez_above,
        ez,
    )
    new_z = both(
        lambda h, y_up, y, x_up, x_: keep * h + gain * ((y_up - y) - (x_up - x_)),
        hz,
        ey_above,
        ey,
        next_y(ex, cosine, sine),
        ex,
    )
    store_couple(h_ref, new_x, 0, x)
    store_couple(h_ref, new_y, 1, x)
    store_couple(h_ref, new_z, 2, x)


def new_e(e, h, hy_below, hz_below, retain, factor, sheet, drive, cosine, sine):
    ex, ey, ez = e
    hx, hy, hz = h
    drive_x = both(lambda s: drive * s, sheet)
    new_x = scaled(
        (retain, factor),
        lambda r, f, e_, z, z_dn, y, y_dn, s: r * e_ + f * ((z - z_dn) - (y - y_dn) - s),
        ex,
        hz,
        prior_y(hz, cosine, sine),
        hy,
        prior_z(hy),
        drive_x,
    )
    new_y = scaled(
        (retain, factor),
        lambda r, f, e_, x, x_dn, z, z_dn: r * e_ + f * ((x - x_dn) - (z - z_dn)),
        ey,
        hx,
        prior_z(hx),
        hz,
        hz_below,
    )
    new_z = scaled(
        (retain, factor),
        lambda r, f, e_, y, y_dn, x, x_dn: r * e_ + f * ((y - y_dn) - (x - x_dn)),
        ez,
        hy,
        hy_below,
        hx,
        prior_y(hx, cosine, sine),
    )
    return new_x, new_y, new_z


def e_row(e_ref, h_ref, c_ref, sheet_ref, x, drive, cosine, sine, below=None):
    e = [load_couple(e_ref, m, x) for m in range(3)]
    h = [load_couple(h_ref, m, x) for m in range(3)]
    if below is None:
        below = [load_couple(h_ref, m, x - 1) for m in (1, 2)]
    retain, factor = load(c_ref, 0, x), load(c_ref, 1, x)
    sheet = (load(sheet_ref, 0, x), load(sheet_ref, 1, x))
    new = new_e(e, h, *below, retain, factor, sheet, drive, cosine, sine)
    for m in range(3):
        store_couple(e_ref, new[m], m, x)
    return new


def is_upper(phase):
    return lax.axis_index("sp") % 2 == phase


def fetch(pairs, sems):
    copies = [
        pltpu.make_async_copy(source, target, sems.at[i])
        for i, (source, target) in enumerate(pairs)
    ]
    for copy in copies:
        copy.start()
    return copies


def first_kernel(
    bloch_hbm, peak_hbm, wave_hbm, e_hbm, h_hbm, p_ref, one_ref, two_ref,
    bloch, peak, wave, low, high, mag, sems,
):
    rows = e_hbm.shape[1]
    copies = fetch(
        [
            (bloch_hbm, bloch),
            (peak_hbm, peak),
            (wave_hbm, wave),
            (e_hbm.at[pl.ds(2, 4), 0], low),
            (e_hbm.at[:, rows - 1], high),
            (h_hbm.at[pl.ds(2, 4), rows - 1], mag),
        ],
        sems,
    )
    for copy in copies[:3]:
        copy.wait()
    shape = p_ref.shape[1:]
    angle_x, angle_y = (
        2.0 * jnp.pi * jnp.full(shape, bloch[0, axis].astype(F32)) / MPHASE
        for axis in range(2)
    )
    cos_x, sin_x = jnp.cos(angle_x), jnp.sin(angle_x)
    slab, slabs = lax.axis_index("sp"), lax.axis_size("sp")
    at_end, at_start = slab == slabs - 1, slab == 0
    half = conductivity(peak[0], shape) * (0.5 * TIME_STEP)
    p_ref[COS] = cosine = jnp.cos(angle_y)
    p_ref[SIN] = sine = jnp.sin(angle_y)
    p_ref[END] = jnp.where(at_end, cos_x, 1.0)
    p_ref[END + 1] = jnp.where(at_end, sin_x, 0.0)
    p_ref[START] = jnp.where(at_start, cos_x, 1.0)
    p_ref[START + 1] = jnp.where(at_start, -sin_x, 0.0)
    p_ref[KEEP] = keep = (1.0 - half) / (1.0 + half)
    p_ref[GAIN] = gain = -TIME_STEP / (1.0 + half)
    for step in range(wave.shape[0]):
        p_ref[DRIVE + step] = jnp.full(shape, wave[step])
    for copy in copies[3:]:
        copy.wait()

    def write(d_ref, s_ref):
        d_ref[...] = low[...].astype(F32)
        ex, ey, ez = (load_couple(high, m) for m in range(3))
        hy, hz = (load_couple(mag, m) for m in range(2))
        part_y, part_z = partial_h(ex, ey, ez, hy, hz, keep, gain, cosine, sine)
        store_couple(s_ref, part_y, 0)
        store_couple(s_ref, part_z, 1)

    @pl.when(is_upper(0))
    def _():
        write(two_ref, one_ref)

    @pl.when(jnp.logical_not(is_upper(0)))
    def _():
        write(one_ref, two_ref)


def widen_kernel(
    peak_hbm, perm_hbm, mat_hbm, e_hbm, h_hbm, e_ref, h_ref, c_ref,
    peak, perm, mat, e_in, h_in, small, sems,
):
    rows, width, depth = mat.shape
    parts = sems.shape[0]
    size = rows // parts
    scalars = fetch([(peak_hbm, peak), (perm_hbm, perm)], small)
    copies = []
    for part in range(parts):
        some = pl.ds(part * size, size)
        copies.append(
            fetch(
                [
                    (mat_hbm.at[some], mat.at[some]),
                    (e_hbm.at[:, some], e_in.at[:, some]),
                    (h_hbm.at[:, some], h_in.at[:, some]),
                ],
                sems.at[part],
            )
        )
    for copy in scalars:
        copy.wait()
    conduct = conductivity(peak[0], (SUB, depth)) * (0.5 * TIME_STEP)
    levels = []
    for index in range(NMAT):
        half = conduct / perm[index]
        levels.append(
            ((1.0 - half) / (1.0 + half), TIME_STEP / perm[index] / (1.0 + half))
        )

    def one_row(x, carry):
        for j in range(width // SUB):
            tile = pl.ds(SUB * j, SUB)
            level = mat[x, tile]
            retain, factor = levels[0]
            for index in range(1, NMAT):
                retain = jnp.where(level == index, levels[index][0], retain)
                factor = jnp.where(level == index, levels[index][1], factor)
            c_ref[0, x, tile] = retain
            c_ref[1, x, tile] = factor
        for m in range(6):
            e_ref[m, x] = e_in[m, x].astype(F32)
            h_ref[m, x] = h_in[m, x].astype(F32)
        return carry

    for part in range(parts):
        for copy in copies[part]:
            copy.wait()
        lax.fori_loop(part * size, (part + 1) * size, one_row, 0)


def conductivity(peak, shape):
    depth = shape[-1]
    height = lax.broadcasted_iota(jnp.int32, shape, len(shape) - 1).astype(F32)
    low = jnp.maximum(PML - height, 0.0) / PML
    high = jnp.maximum(height - (depth - 1 - PML), 0.0) / PML
    return peak * (low * low * low + high * high * high)


def inner_kernel(phase, step, p_ref, c_ref, sheet_ref, e_in, h_in, e_ref, h_ref):
    rows = e_ref.shape[1]
    middle = rows // 2
    cosine, sine, drive = p_ref[COS], p_ref[SIN], p_ref[DRIVE + step]
    keep, gain = p_ref[KEEP], p_ref[GAIN]
    upper = is_upper(phase)
    lo = jnp.where(upper, middle, 0)
    hi = jnp.where(upper, rows - 1, middle)
    skip = 1 if phase == 0 else jnp.where(upper, 0, 1)

    def new_h(x):
        h_row(e_ref, h_ref, x, keep, gain, cosine, sine)

    def new_electric(x):
        e_row(e_ref, h_ref, c_ref, sheet_ref, x, drive, cosine, sine)

    def start_row(x, carry):
        new_h(x)
        return carry

    def one_row(x, carry):
        new_h(x + 1)
        new_electric(x)
        return carry

    lax.fori_loop(lo, lo + skip + 1, start_row, 0)
    begin = lo + skip
    pairs = (hi - 1 - begin) // 2

    def two_rows(pair, carry):
        one_row(begin + 2 * pair, carry)
        return one_row(begin + 2 * pair + 1, carry)

    lax.fori_loop(0, pairs, two_rows, 0)
    lax.fori_loop(begin + 2 * pairs, hi - 1, one_row, 0)
    new_electric(hi - 1)

    @pl.when(upper)
    def _():
        ey, ez = (load_couple(e_ref, m, rows - 1) for m in (1, 2))
        hx = load_couple(h_ref, 0, rows - 1)
        store_couple(h_ref, new_hx(ey, ez, hx, keep, gain, cosine, sine), 0, rows - 1)

    if phase == 1:

        @pl.when(jnp.logical_not(upper))
        def _():
            new_electric(middle)


def edge_step(
    phase, step, p_ref, c_ref, sheet_ref, mine_ref, their_ref, e_ref, h_ref, out_ref=None
):
    cosine, sine, drive = p_ref[COS], p_ref[SIN], p_ref[DRIVE + step]
    keep, gain = p_ref[KEEP], p_ref[GAIN]
    top = e_ref.shape[1] - 1
    upper = is_upper(phase)

    @pl.when(upper)
    def _():
        part_y, part_z = (load_couple(mine_ref, m) for m in range(2))
        ey_above, ez_above = (
            turn(load_couple(their_ref, m), p_ref[END], p_ref[END + 1]) for m in range(2)
        )
        hy, hz = close_h(part_y, part_z, ey_above, ez_above, gain)
        store_couple(h_ref, hy, 1, top)
        store_couple(h_ref, hz, 2, top)
        ex, ey, ez = e_row(e_ref, h_ref, c_ref, sheet_ref, top, drive, cosine, sine)
        if out_ref is not None:
            part_y, part_z = partial_h(ex, ey, ez, hy, hz, keep, gain, cosine, sine)
            store_couple(out_ref, part_y, 0)
            store_couple(out_ref, part_z, 1)

    @pl.when(jnp.logical_not(upper))
    def _():
        part_y, part_z = (
            turn(load_couple(their_ref, m), p_ref[START], p_ref[START + 1])
            for m in range(2)
        )
        ey, ez = (load_couple(e_ref, m, 0) for m in (1, 2))
        below = close_h(part_y, part_z, ey, ez, gain)
        _, ey, ez = e_row(
            e_ref, h_ref, c_ref, sheet_ref, 0, drive, cosine, sine, below
        )
        if out_ref is not None:
            store_couple(out_ref, ey, 0)
            store_couple(out_ref, ez, 1)


def edge_kernel(
    phase, step, p_ref, c_ref, sheet_ref, mine_ref, their_ref, e_in, h_in,
    e_ref, h_ref, *out_ref,
):
    edge_step(
        phase, step, p_ref, c_ref, sheet_ref, mine_ref, their_ref, e_ref, h_ref, *out_ref
    )


def last_kernel(
    phase, step, slot, scale, p_ref, c_ref, sheet_ref, mine_ref, their_ref, old_ref,
    e_in, h_in, e_ref, h_ref, out_ref,
):
    edge_step(phase, step, p_ref, c_ref, sheet_ref, mine_ref, their_ref, e_ref, h_ref)
    total = jnp.zeros(old_ref.shape, F32)
    ends = [load(e_ref, m, x) for x in (0, e_ref.shape[1] - 1) for m in range(4)]
    for tiles in zip(*ends):
        total = total + sum(tile * tile for tile in tiles)
    out_ref[...] = old_ref[...] + monitor(total, slot, scale)


def monitor(total, slot, scale):
    lanes = lax.broadcasted_iota(jnp.int32, total.shape, 1)
    total = jnp.where(lanes == PML + 6, total, 0.0)
    total = jnp.sum(jnp.sum(total, 0, keepdims=True), 1, keepdims=True) * scale
    return jnp.where(lanes == slot, total, 0.0)


def power_kernel(phase, slot, scale, e_ref, old_ref, out_ref):
    rows, _, depth = e_ref.shape[1:]
    lo, hi = 1, rows - 1
    if phase is not None:
        middle, upper = rows // 2, is_upper(phase)
        lo = jnp.where(upper, middle + (1 - phase), 0)
        hi = jnp.where(upper, rows, middle + phase)

    def one_row(x, sums):
        parts = [load(e_ref, m, x) for m in range(4)]
        return tuple(
            total + ((a * a + b * b) + (c * c + d * d))
            for total, a, b, c, d in zip(sums, *parts)
        )

    zeros = (jnp.zeros((SUB, depth), F32),) * (e_ref.shape[-2] // SUB)
    total = sum(lax.fori_loop(lo, hi, one_row, zeros))
    out_ref[...] = old_ref[...] + monitor(total, slot, scale)


def out_kernel(in_ref, out_ref, sems):
    for copy in fetch([(in_ref, out_ref)], sems):
        copy.wait()


def add_kernel(scale, *refs):
    total = refs[0][...]
    for ref in refs[1:-1]:
        total = total + ref[...]
    refs[-1][...] = total * scale if scale != 1.0 else total


def call(kernel, outs, ins, specs, aliases=None, scratch=(), flops=0, vmem=16):
    return pl.pallas_call(
        kernel,
        out_shape=tuple(pltpu.VMEM(shape, F32) for shape in outs),
        in_specs=specs,
        out_specs=tuple(VMEM for _ in outs),
        input_output_aliases=aliases or {},
        scratch_shapes=scratch,
        cost_estimate=pl.CostEstimate(flops=flops, bytes_accessed=0, transcendentals=0),
        compiler_params=pltpu.CompilerParams(vmem_limit_bytes=vmem * 2**20),
    )(*ins)


def swap(value, phase):
    count = lax.axis_size("sp")
    pairs = [(i, (((i - phase) % count ^ 1) + phase) % count) for i in range(count)]
    return lax.ppermute(value, "sp", pairs)


def shift(value, axis, steps):
    count = lax.axis_size(axis)
    return lax.ppermute(value, axis, [(i, (i + steps) % count) for i in range(count)])


def total_over(value, axis, scale=1.0):
    count = lax.axis_size(axis)
    shape = value.shape
    if count & (count - 1):
        parts = [value] + [shift(value, axis, step) for step in range(1, count)]
        return call(functools.partial(add_kernel, scale), [shape], parts, [VMEM] * count)[0]
    step = 1
    while step < count:
        other = lax.ppermute(value, axis, [(i, i ^ step) for i in range(count)])
        step *= 2
        last = scale if step >= count else 1.0
        value = call(
            functools.partial(add_kernel, last), [shape], [value, other], [VMEM] * 2
        )[0]
    return value


def to_hbm(value):
    return pl.pallas_call(
        out_kernel,
        out_shape=jax.ShapeDtypeStruct(value.shape, F32),
        in_specs=[VMEM],
        out_specs=HBM,
        scratch_shapes=[pltpu.SemaphoreType.DMA((1,))],
        compiler_params=pltpu.CompilerParams(vmem_limit_bytes=2**20),
    )(value)


def on_device(
    bloch_index,
    material,
    permittivity,
    absorption_peak,
    source_sheet,
    waveform,
    electric_in,
    magnetic_in,
):
    points = bloch_index.shape[0]
    rows, width, depth = material.shape
    total_points = points * lax.axis_size("ka")
    cells_plane = rows * lax.axis_size("sp") * width
    plane = (jnp.arange(depth) == PML + 2).astype(F32)
    sheets = source_sheet[..., None] * plane
    results = [
        one_point(
            bloch_index[point : point + 1], sheets[point], waveform, material, permittivity,
            absorption_peak, electric_in[point], magnetic_in[point], 1.0 / cells_plane,
        )
        for point in range(points)
    ]
    electric, magnetic, powers = zip(*results)
    sums = [total_over(power, "sp") for power in powers]
    electric = [to_hbm(value) for value in electric]
    local = sums[0]
    for other in sums[1:]:
        local = local + other
    mean = total_over(local, "ka", 1.0 / total_points)
    magnetic = [to_hbm(value) for value in magnetic]
    return (
        jnp.stack(electric),
        jnp.stack(magnetic),
        jnp.stack([total[0, :NSNAP] for total in sums]),
        mean[0, :NSNAP],
    )


def one_point(
    bloch, sheet, waveform, material, permittivity, peak, electric_in, magnetic_in, scale
):
    rows, width, depth = material.shape
    steps = waveform.shape[0]
    edge = (4, width, depth)
    full = (6, rows, width, depth)
    dtype = electric_in.dtype
    bloch, waveform, permittivity, electric_in, magnetic_in, material = (
        pltpu.with_memory_space_constraint(value, pltpu.HBM)
        for value in (bloch, waveform, permittivity, electric_in, magnetic_in, material)
    )
    p, *mine = call(
        first_kernel,
        [(DRIVE + steps, SUB, depth), edge, edge],
        [bloch, peak, waveform, electric_in, magnetic_in],
        [HBM, ANY] + [HBM] * 3,
        scratch=[
            pltpu.SMEM(bloch.shape, bloch.dtype),
            pltpu.SMEM(peak.shape, F32),
            pltpu.SMEM(waveform.shape, F32),
            pltpu.VMEM((4, width, depth), dtype),
            pltpu.VMEM((6, width, depth), dtype),
            pltpu.VMEM((4, width, depth), dtype),
            pltpu.SemaphoreType.DMA((6,)),
        ],
    )
    their = [swap(mine[phase], phase) for phase in range(2)]
    e, h, c = call(
        widen_kernel,
        [full, full, (2, rows, width, depth)],
        [peak, permittivity, material, electric_in, magnetic_in],
        [ANY] + [HBM] * 4,
        scratch=[
            pltpu.SMEM(peak.shape, F32),
            pltpu.SMEM(permittivity.shape, F32),
            pltpu.VMEM(material.shape, material.dtype),
            pltpu.VMEM(full, dtype),
            pltpu.VMEM(full, dtype),
            pltpu.SemaphoreType.DMA((2,)),
            pltpu.SemaphoreType.DMA((4, 3)),
        ],
    )
    power = jnp.zeros((SUB, depth), F32)

    def inner(phase, step, e, h):
        return call(
            functools.partial(inner_kernel, phase, step),
            [full, full],
            [p, c, sheet, e, h],
            [VMEM] * 5,
            {3: 0, 4: 1},
        )

    def measured(phase, step, power, e):
        return call(
            functools.partial(power_kernel, phase, step // INTERVAL, scale),
            [(SUB, depth)],
            [e, power],
            [VMEM, VMEM],
        )[0]

    e, h = inner(0, 0, e, h)
    for step in range(steps - 1):
        for phase in range(2):
            e, h, mine[phase] = call(
                functools.partial(edge_kernel, phase, step),
                [full, full, edge],
                [p, c, sheet, mine[phase], their[phase], e, h],
                [VMEM] * 7,
                {5: 0, 6: 1},
            )
            if (step + 1) % INTERVAL == 0:
                power = measured(phase, step, power, e)
            their[phase] = swap(mine[phase], phase)
            if step == phase == 0:
                e, h = inner(1, 0, e, h)
            e, h = inner(phase, step + 1, e, h)
    step = steps - 1
    power = measured(None, step, power, e)
    e, h = call(
        functools.partial(edge_kernel, 0, step),
        [full, full],
        [p, c, sheet, mine[0], their[0], e, h],
        [VMEM] * 7,
        {5: 0, 6: 1},
    )
    e, h, power = call(
        functools.partial(last_kernel, 1, step, step // INTERVAL, scale),
        [full, full, (SUB, depth)],
        [p, c, sheet, mine[1], their[1], power, e, h],
        [VMEM] * 8,
        {6: 0, 7: 1},
    )
    return e, h, power


def solution(mesh):
    in_specs = (
        P("ka", None),
        P("sp", None, None),
        P(),
        P(),
        P("ka", None, "sp", None),
        P(),
        P("ka", None, "sp", None, None),
        P("ka", None, "sp", None, None),
    )
    out_specs = (
        P("ka", None, "sp", None, None),
        P("ka", None, "sp", None, None),
        P("ka", None),
        P(),
    )
    return jax.shard_map(
        on_device, mesh=mesh, in_specs=in_specs, out_specs=out_specs, check_vma=False
    )
```
